128 devices in a mesh: tp: 8 (over z_hi, x), seq: 16 (over y, z_lo, core).
Axes of the slice: x: 4, y: 4, z: 4 (z_hi: 2, z_lo: 2; z = z_hi * 2 + z_lo), core: 2. Of those that a mesh axis runs over, the one named last changes fastest.
Arguments:
- query_rows: bfloat16 [4096, 8192], P('seq', 'tp'), may hold values from -24 to 24
- key_rows: bfloat16 [4096, 1024], P('seq', 'tp'), may hold values from -9 to 9
- value_rows: bfloat16 [4096, 1024], P('seq', 'tp'), may hold values from -9 to 9
- mixer_input: bfloat16 [4096, 8192], P('seq', 'tp'), may hold values from -6 to 6
- write_rows: bfloat16 [4096, 128], P('seq'), may hold values from -48 to 48
- read_rows: bfloat16 [4096, 128], P('seq'), may hold values from -48 to 48
- log_step: float32 [128, 4096], P('tp', 'seq'), may hold values from -20 to -4
- log_decay: float32 [128, 4096], P('tp', 'seq'), may hold values from -2 to 0
Outputs:
- grad_input: float32 [4096, 8192], P('seq', 'tp')
- grad_write: float32 [4096, 128], P('seq')
- grad_read: float32 [4096, 128], P('seq')
- grad_log_step: float32 [128, 4096], P('tp', 'seq')
The draws below stay inside these ranges and needn't reach their ends.
All inputs are finite; a program needn't handle non-finite values.
Results may differ from the reference program's by a relative error of at most 0.0015.
Values may be sent and summed in bfloat16 or wider, within the bound.
A program may use at most 128 MiB of HBM per device.

```python
import math
import jax
import jax.numpy as jnp
from jax import lax

BLOCK = 128
HQ = 64
KV = 8
HD = 128
H = 128
P_SIZE = 64
N = 128
SEQ_LEN = 4096


def teacher_keys(key):
    length = SEQ_LEN
    columns = KV * HD
    normal_base = jax.random.normal(jax.random.fold_in(key, 11), (length, columns), jnp.float32)
    keys_drawn = jnp.clip(1.4 * normal_base, -8.4, 8.4)
    return keys_drawn


def draw_key_rows(key, part):
    return teacher_keys(key).astype(jnp.bfloat16)


def draw_query_rows(key, part):
    normal_base = jax.random.normal(jax.random.fold_in(key, 14), (SEQ_LEN, HQ * HD), jnp.float32)
    drawn = jnp.clip(1.4 * normal_base, -8.4, 8.4)
    return drawn.astype(jnp.bfloat16)


def head_rates(key):
    picked = jax.random.randint(jax.random.fold_in(key, 21), (H,), 0, 16)
    slow_heads = picked < 11
    slow_rate = jnp.exp(jax.random.uniform(jax.random.fold_in(key, 26), (H,), jnp.float32, math.log(0.05), math.log(0.6))) / SEQ_LEN
    fast_rate = jnp.exp(jax.random.uniform(jax.random.fold_in(key, 27), (H,), jnp.float32, math.log(0.02), math.log(0.033)))
    return jnp.where(slow_heads, slow_rate, fast_rate)


def draw_log_decay(key, part):
    rates = head_rates(key)
    rough = jnp.exp(jax.random.uniform(jax.random.fold_in(key, 22), (H, SEQ_LEN), jnp.float32, math.log(0.5), math.log(2.0)))
    drawn = -rates[:, None] * rough
    spots = jax.random.randint(jax.random.fold_in(key, 23), (3,), 0, SEQ_LEN)
    amount = jnp.exp(jax.random.uniform(jax.random.fold_in(key, 24), (H, 3), jnp.float32, math.log(0.2), math.log(0.5)))
    return drawn.at[:, spots].add(-amount)


def draw_log_step(key, part):
    rates = head_rates(key)
    rough = jnp.exp(jax.random.uniform(jax.random.fold_in(key, 25), (H, SEQ_LEN), jnp.float32, math.log(0.5), math.log(2.0)))
    factor = 1.0 / (64.0 * math.sqrt(N))
    return jnp.log(factor * jnp.sqrt(rates)[:, None] * rough)


def level_of(key, shape, shards, smallest, top_value):
    factor_of, own = 1.0, jax.random.fold_in(key, 6)
    for dim, shards_of in shards:
        steps = jnp.exp(jax.random.uniform(jax.random.fold_in(own, dim), (shards_of,), jnp.float32, smallest / len(shards), top_value / len(shards)))
        factor_of = factor_of * jnp.repeat(steps, shape[dim] // shards_of).reshape([-1 if axis == dim else 1 for axis in range(len(shape))])
    return factor_of


def bell_draw(key, extent, scale, limit, split=(), kind=jnp.bfloat16):
    level = level_of(key, extent, split, -0.22, 0.18) if split else 1.0
    values = jax.random.normal(key, extent, jnp.float32) * scale * level
    return jnp.minimum(jnp.maximum(values, -limit), limit).astype(kind)


def setup_inputs(seed: int = 0) -> dict:
    splits = jax.random.split(jax.random.key(seed), 9)
    return {
        "query_rows": draw_query_rows(jax.random.fold_in(splits[8], 71), 0),
        "key_rows": draw_key_rows(jax.random.fold_in(splits[8], 71), 0),
        "value_rows": bell_draw(splits[2], (SEQ_LEN, KV * HD), 1.5, 9.0, ((0, 16), (1, 8))),
        "mixer_input": bell_draw(splits[3], (SEQ_LEN, H * P_SIZE), 1.0, 6.0, ((0, 16), (1, 8))),
        "write_rows": bell_draw(splits[4], (SEQ_LEN, N), 8.0, 48.0, ((0, 16),)),
        "read_rows": bell_draw(splits[5], (SEQ_LEN, N), 8.0, 48.0, ((0, 16),)),
        "log_step": draw_log_step(jax.random.fold_in(splits[8], 71), 0),
        "log_decay": draw_log_decay(jax.random.fold_in(splits[8], 71), 0),
    }


precise = lax.Precision.HIGHEST

def teacher(query_rows, key_rows, value_rows):
    length = query_rows.shape[0]
    group = HQ // KV
    query_heads = jnp.transpose(query_rows.reshape(length, HQ, HD), (1, 0, 2))
    key_heads = jnp.transpose(key_rows.reshape(length, KV, HD), (1, 0, 2))
    value_heads = jnp.transpose(value_rows.reshape(length, KV, HD), (1, 0, 2))
    positions = jnp.arange(length, dtype=jnp.int32)
    allowed = positions[None, :] <= positions[:, None]
    scaling = 1.0 / math.sqrt(HD)

    def one_head(head):
        query_now = query_heads[head]
        key_now = key_heads[head // group]
        value_now = value_heads[head // group]
        scores = jnp.dot(query_now, key_now.T, preferred_element_type=jnp.float32) * scaling
        scores = jnp.where(allowed, scores, -1e+30)
        top_score = lax.optimization_barrier(jnp.max(scores, axis=-1, keepdims=True))
        weights = jnp.where(allowed, jnp.exp(scores - top_score), 0.0)
        totals = lax.optimization_barrier(jnp.sum(weights, axis=-1, keepdims=True))
        mixed = jnp.dot(weights.astype(jnp.bfloat16), value_now, preferred_element_type=jnp.float32)
        return mixed / totals
    output = lax.map(one_head, jnp.arange(HQ, dtype=jnp.int32))
    return jnp.transpose(output, (1, 0, 2)).reshape(length, HQ * HD).astype(jnp.bfloat16)

def student(signal, writes, reads, log_step, log_decay):
    head_count = log_step.shape[0]
    length = signal.shape[0]
    blocks = length // BLOCK
    head_width = signal.shape[1] // head_count
    states = writes.shape[1]
    signal_blocks = signal.reshape(blocks, BLOCK, head_count, head_width)
    write_blocks = writes.reshape(blocks, BLOCK, states)
    read_blocks = reads.reshape(blocks, BLOCK, states)
    step_blocks = jnp.transpose(jnp.exp(log_step).reshape(head_count, blocks, BLOCK), (1, 0, 2))
    decay_blocks = jnp.transpose(log_decay.reshape(head_count, blocks, BLOCK), (1, 0, 2))
    causal = jnp.arange(BLOCK, dtype=jnp.int32)[:, None] >= jnp.arange(BLOCK, dtype=jnp.int32)[None, :]

    def one_block(state, element):
        signal_now, write_now, read_now, step_now, decay_now = element
        cum_decay = jnp.cumsum(decay_now, axis=-1)
        log_gap = cum_decay[:, :, None] - cum_decay[:, None, :]
        within = jnp.where(causal, jnp.exp(jnp.where(causal, log_gap, 0.0)), 0.0)
        inner_rows = jnp.dot(read_now, write_now.T, preferred_element_type=jnp.float32, precision=precise)
        scaled = signal_now * step_now.T[:, :, None]
        y_local = jnp.einsum('hij,jhp->ihp', within * inner_rows[None], scaled, precision=precise)
        y_carried = jnp.einsum('hpn,in->ihp', state, read_now, precision=precise) * jnp.exp(cum_decay).T[:, :, None]
        to_end = jnp.exp(cum_decay[:, -1:] - cum_decay).T
        added = jnp.einsum('jhp,jn->hpn', scaled * to_end[:, :, None], write_now, precision=precise)
        new_state = jnp.exp(cum_decay[:, -1])[:, None, None] * state + added
        return (new_state, y_local + y_carried)
    initial = jnp.zeros((head_count, head_width, states), jnp.float32)
    final_state, outputs = lax.scan(one_block, initial, (signal_blocks, write_blocks, read_blocks, step_blocks, decay_blocks))
    return outputs.reshape(length, head_count * head_width)

def reference(query_rows, key_rows, value_rows, mixer_input, write_rows, read_rows, log_step, log_decay):
    target = teacher(query_rows, key_rows, value_rows)
    signal = mixer_input.astype(jnp.float32)
    writes = write_rows.astype(jnp.float32)
    reads = read_rows.astype(jnp.float32)

    def forward(signal_in, writes_in, reads_in, step_in):
        return student(signal_in, writes_in, reads_in, step_in, log_decay)
    student_out, pullback = jax.vjp(forward, signal, writes, reads, log_step)
    residual = student_out - target.astype(jnp.float32)
    grad_input, grad_write, grad_read, grad_log_step = pullback(residual)
    return (grad_input, grad_write, grad_read, grad_log_step)
```

```python
import functools
import math

import jax
import jax.numpy as jnp
from jax import lax
from jax.experimental import pallas as pl
from jax.experimental.pallas import tpu as pltpu
from jax.sharding import PartitionSpec as P

MESH = pl.DeviceIdType.MESH
F32, BF16 = jnp.float32, jnp.bfloat16
TOK = 256
HD = 128
LOW = -1e30
SEQ = 16
CHIPS = 8
PAIRS = 8
TP = 8
SCALE = math.log2(math.e) / math.sqrt(HD)


def dot(a, b):
    return jnp.dot(a, b, preferred_element_type=F32)


def dot_nt(a, b):
    return lax.dot_general(a, b, (((1,), (1,)), ((), ())), preferred_element_type=F32)


def halves(a):
    high = a.astype(BF16)
    return high, (a - high.astype(F32)).astype(BF16)


def three(op, a, b):
    (ah, al), (bh, bl) = halves(a), halves(b)
    return op(ah, bh) + op(al, bh) + op(ah, bl)


def remote(src, dst, send_sem, recv_sem, axis, index):
    return pltpu.make_async_remote_copy(
        src_ref=src,
        dst_ref=dst,
        send_sem=send_sem,
        recv_sem=recv_sem,
        device_id={axis: index},
        device_id_type=MESH,
    )


def main_kernel(
    q_ref,
    k_ref,
    v_ref,
    x_ref,
    w_ref,
    r_ref,
    ls_ref,
    ld_ref,
    gi_ref,
    gwr_ref,
    gls_ref,
    keys,
    values,
    scores,
    peak,
    total,
    mixed,
    decay_buf,
    mix_high,
    mix_low,
    from_start,
    in_scale,
    local_y,
    back,
    wt_buf,
    rt_buf,
    pair_buf,
    lane_decay,
    fwd_local,
    fwd_sibling,
    fwd_chip,
    fwd_got,
    fwd_out,
    fwd_in,
    state_in,
    bwd_local,
    bwd_sibling,
    bwd_chip,
    bwd_got,
    bwd_out,
    bwd_in,
    key_send,
    key_recv,
    value_send,
    value_recv,
    sib_send,
    sib_recv,
    leg_send,
    leg_recv,
    ret_send,
    ret_recv,
):
    me = lax.axis_index("seq")
    core = lax.rem(me, 2)
    chip = me // 2
    sibling = me + 1 - 2 * core
    partner = me + 2 - 4 * lax.rem(chip, 2)
    above = lax.rem(me + 4, SEQ)
    below = lax.rem(me + 12, SEQ)
    far = lax.rem(me + 8, SEQ)
    above_p, below_p = lax.rem(partner + 4, SEQ), lax.rem(partner + 12, SEQ)
    far_p = lax.rem(partner + 8, SEQ)
    started = []

    barrier = pltpu.get_barrier_semaphore()
    for hop in range(1, SEQ):
        pl.semaphore_signal(
            barrier,
            inc=1,
            device_id={"seq": lax.rem(me + hop, SEQ)},
            device_id_type=MESH,
        )

    log_decay = ld_ref[...]
    log_step = ls_ref[...]
    rows = lax.broadcasted_iota(jnp.int32, (TOK, TOK), 0)
    cols = lax.broadcasted_iota(jnp.int32, (TOK, TOK), 1)
    causal = rows >= cols
    upper = jnp.where(rows <= cols, 1.0, 0.0).astype(BF16)
    d1 = log_decay.astype(BF16)
    rest = log_decay - d1.astype(F32)
    d2 = rest.astype(BF16)
    d3 = (rest - d2.astype(F32)).astype(BF16)
    cum = dot(d1, upper) + dot(d2, upper) + dot(d3, upper)
    end = cum[:, TOK - 1 : TOK]
    row_term = log_step - cum
    log_in = row_term + end
    columns = jnp.concatenate([cum, log_in, jnp.zeros((96, TOK), F32)], axis=0).T
    lane = lax.broadcasted_iota(jnp.int32, (TOK, HD), 1)
    first = lane < 64
    lane8 = lax.broadcasted_iota(jnp.int32, (8, HD), 1)
    wt_buf[...] = w_ref[...].T
    rt_buf[...] = r_ref[...].T
    for t in range(PAIRS):
        a, b = 2 * t, 2 * t + 1
        at = slice(t * HD, (t + 1) * HD)
        from_start[:, at] = jnp.exp(
            jnp.where(first, columns[:, a : a + 1], columns[:, b : b + 1])
        )
        scale = jnp.exp(
            jnp.where(first, columns[:, 16 + a : 17 + a], columns[:, 16 + b : 17 + b])
        )
        in_scale[:, at] = scale
        tile = jnp.where(lane8 < 64, end[a : a + 1, :], end[b : b + 1, :])
        lane_decay[t] = tile
        high, low = halves(x_ref[:, at].astype(F32) * scale)
        state = dot(wt_buf[...], high) + dot(wt_buf[...], low)
        for half in range(2):
            fwd_local[t, half, 0:64] = state[half * 64 : (half + 1) * 64]
            fwd_local[t, half, 64:72] = tile

    pl.semaphore_wait(barrier, SEQ - 1)

    def begin(copy):
        copy.start()
        started.append(copy)

    count = [0]

    def pass_block(source, index, target):
        n = count[0]
        count[0] += 1
        src_k = k_ref if source is None else keys.at[index]
        src_v = v_ref if source is None else values.at[index]
        begin(remote(src_k, keys.at[index], key_send.at[n], key_recv.at[index], "seq", target))
        begin(
            remote(src_v, values.at[index], value_send.at[n], value_recv.at[index], "seq", target)
        )

    def await_block(index):
        remote(
            keys.at[index], keys.at[index], key_send.at[0], key_recv.at[index], "seq", sibling
        ).wait_recv()
        remote(
            values.at[index], values.at[index], value_send.at[0], value_recv.at[index], "seq", sibling
        ).wait_recv()

    for target in (partner, above, below, sibling):
        pass_block(None, me, target)
    begin(remote(fwd_local, fwd_sibling, sib_send.at[0], sib_recv.at[0], "seq", sibling))
    keys[me] = k_ref[...]
    values[me] = v_ref[...]

    inner = dot_nt(r_ref[...], w_ref[...])

    def build(h):
        gap = columns[:, h : h + 1] + row_term[h : h + 1, :]
        decay = jnp.where(causal, jnp.exp(gap), 0.0)
        decay_buf[h] = decay
        high, low = halves(decay * inner)
        mix_high[h] = high
        mix_low[h] = low

    for h in range(8):
        build(h)

    def chip_states(local, sib, out, early_first):
        for t in range(PAIRS):
            mine, other = local[t, core], sib[t, core]
            early = jnp.where(core == 0, mine, other)
            late = jnp.where(core == 0, other, mine)
            if not early_first:
                early, late = late, early
            out[t, 0:64] = early[0:64] * jnp.exp(late[64:65]) + late[0:64]
            out[t, 64:72] = early[64:72] + late[64:72]

    def send_leg(stage, chip_buf, got):
        got[chip] = chip_buf[chip]
        for hop in range(1, CHIPS):
            target = lax.rem(chip + hop, CHIPS)
            begin(
                remote(
                    chip_buf.at[target],
                    got.at[chip],
                    leg_send.at[stage, hop],
                    leg_recv.at[stage, chip],
                    "seq",
                    2 * target + core,
                )
            )

    def scan_leg(stage, got, out, into, order):
        for hop in range(1, CHIPS):
            source = lax.rem(chip + hop, CHIPS)
            remote(
                got.at[source],
                got.at[source],
                leg_send.at[stage, 0],
                leg_recv.at[stage, source],
                "seq",
                sibling,
            ).wait_recv()
        running = jnp.zeros((64, HD), F32)
        for i in order:
            out[i] = running
            running = running * jnp.exp(got[i, 64:65]) + got[i, 0:64]
        into[core, chip] = out[chip]
        for hop in range(1, CHIPS):
            target = lax.rem(chip + hop, CHIPS)
            begin(
                remote(
                    out.at[target],
                    into.at[core, chip],
                    ret_send.at[stage, hop],
                    ret_recv.at[stage, chip],
                    "seq",
                    2 * target + core,
                )
            )

    def spread(stage, into):
        for hop in range(1, CHIPS):
            source = lax.rem(chip + hop, CHIPS)
            remote(
                into.at[core, source],
                into.at[core, source],
                ret_send.at[stage, 0],
                ret_recv.at[stage, source],
                "seq",
                sibling,
            ).wait_recv()
        begin(
            remote(
                into.at[core],
                into.at[core],
                sib_send.at[2 * stage + 1],
                sib_recv.at[2 * stage + 1],
                "seq",
                sibling,
            )
        )
        remote(
            into.at[1 - core],
            into.at[1 - core],
            sib_send.at[2 * stage + 1],
            sib_recv.at[2 * stage + 1],
            "seq",
            sibling,
        ).wait_recv()

    remote(
        fwd_sibling, fwd_sibling, sib_send.at[0], sib_recv.at[0], "seq", sibling
    ).wait_recv()
    chip_states(fwd_local, fwd_sibling, fwd_chip, True)
    send_leg(0, fwd_chip, fwd_got)

    await_block(partner)
    for target in (above, below, sibling):
        pass_block(keys, partner, target)

    for h in range(8, 16):
        build(h)

    await_block(below)
    for target in (above, sibling):
        pass_block(keys, below, target)
    await_block(above_p)
    for target in (below, sibling):
        pass_block(keys, above_p, target)

    scan_leg(0, fwd_got, fwd_out, fwd_in, range(CHIPS))

    def make_y(t, carry):
        at = pl.ds(pl.multiple_of(t * HD, HD), HD)
        x = x_ref[:, at]
        xa = jnp.where(first, x, jnp.zeros_like(x))
        xb = jnp.where(first, jnp.zeros_like(x), x)
        local_y[:, at] = (
            dot(mix_high[2 * t], xa)
            + dot(mix_low[2 * t], xa)
            + dot(mix_high[2 * t + 1], xb)
            + dot(mix_low[2 * t + 1], xb)
        )
        return carry

    lax.fori_loop(0, PAIRS, make_y, 0)

    for index in (above, below_p, far, far_p):
        await_block(index)
        pass_block(keys, index, sibling)
    for index in (me, partner, above, below, above_p, below_p, far, far_p):
        await_block(index + 1 - 2 * core)

    peak[...] = jnp.full(peak.shape, LOW, F32)

    def score_block(b, mask):
        kt = keys[b].T
        for h in range(8):
            at = slice(h * TOK, (h + 1) * TOK)
            s = dot(q_ref[:, h * HD : (h + 1) * HD], kt)
            if mask:
                s = jnp.where(causal, s, LOW)
            scores[b, at] = s
            peak[at] = jnp.maximum(peak[at], jnp.maximum(s[:, :HD], s[:, HD:]))

    def score_step(b, carry):
        score_block(b, False)
        return carry

    lax.fori_loop(0, me, score_step, 0)
    score_block(me, True)

    @pl.when(core == 0)
    def _():
        scores[me + 1] = jnp.full((8 * TOK, TOK), LOW, F32)

    spread(0, fwd_in)
    pair_buf[...] = jnp.zeros(pair_buf.shape, F32)
    gwr_ref[...] = jnp.zeros(gwr_ref.shape, F32)

    def group(g, carry):
        at2 = pl.ds(pl.multiple_of(g * 2 * TOK, 2 * TOK), 2 * TOK)
        top = jnp.max(peak[at2], axis=1, keepdims=True) * SCALE
        total[...] = jnp.zeros(total.shape, F32)
        mixed[...] = jnp.zeros(mixed.shape, F32)

        def chunk(n, inner_carry):
            for b in (2 * n, 2 * n + 1):
                weights = jnp.exp2(scores[b, at2] * SCALE - top)
                total[...] += weights[:, :HD] + weights[:, HD:]
                mixed[...] += dot(weights.astype(BF16), values[b])
            return inner_carry

        lax.fori_loop(0, chip + 1, chunk, 0)
        ratio = mixed[...] / jnp.sum(total[...], axis=1, keepdims=True)
        taught = ratio.astype(BF16).astype(F32)
        for part in range(2):
            t = 2 * g + part
            at = pl.ds(pl.multiple_of(t * HD, HD), HD)
            entering = jnp.concatenate([fwd_in[0, t], fwd_in[1, t]], axis=0)
            sib = fwd_sibling[t]
            sib_state = jnp.concatenate([sib[0, 0:64], sib[1, 0:64]], axis=0)
            entering = jnp.where(
                core == 1, entering * jnp.exp(sib[0, 64:65]) + sib_state, entering
            )
            state_in[t] = entering
            sh, sl = halves(entering)
            starts = from_start[:, at]
            carried = (dot(r_ref[...], sh) + dot(r_ref[...], sl)) * starts
            residual = local_y[:, at] + carried - taught[part * TOK : (part + 1) * TOK]
            local_y[:, at] = residual
            wh, wl = halves(residual * starts)
            adjoint = dot(rt_buf[...], wh) + dot(rt_buf[...], wl)
            for half in range(2):
                bwd_local[t, half, 0:64] = adjoint[half * 64 : (half + 1) * 64]
                bwd_local[t, half, 64:72] = lane_decay[t]
        return carry

    lax.fori_loop(0, PAIRS // 2, group, 0)

    begin(remote(bwd_local, bwd_sibling, sib_send.at[2], sib_recv.at[2], "seq", sibling))
    remote(
        bwd_sibling, bwd_sibling, sib_send.at[2], sib_recv.at[2], "seq", sibling
    ).wait_recv()
    chip_states(bwd_local, bwd_sibling, bwd_chip, False)
    send_leg(1, bwd_chip, bwd_got)

    def local_terms(t, carry):
        at = pl.ds(pl.multiple_of(t * HD, HD), HD)
        residual = local_y[:, at]
        xt = x_ref[:, at].T
        for part, own in ((0, first), (1, ~first)):
            rh, rl = halves(jnp.where(own, residual, 0.0))
            pair_buf[...] += decay_buf[2 * t + part] * (dot(rh, xt) + dot(rl, xt))
        return carry

    def back_terms(t, carry):
        at = pl.ds(pl.multiple_of(t * HD, HD), HD)
        residual_t = local_y[:, at].T
        rh, rl = halves(residual_t)
        pieces = []
        for part in range(2):
            own = slice(part * 64, (part + 1) * 64)
            both = jnp.concatenate([rh[own], rl[own]], axis=0)
            product = dot(both, mix_high[2 * t + part])
            pieces.append(product[0:64] + product[64:128] + dot(rh[own], mix_low[2 * t + part]))
        back[:, at] = jnp.concatenate(pieces, axis=0).T
        return carry

    def read_terms(t, carry):
        at = pl.ds(pl.multiple_of(t * HD, HD), HD)
        weighted = local_y[:, at] * from_start[:, at]
        gwr_ref[TOK : 2 * TOK] += three(dot_nt, weighted, state_in[t])
        return carry

    lax.fori_loop(0, PAIRS, local_terms, 0)
    scan_leg(1, bwd_got, bwd_out, bwd_in, range(CHIPS - 1, -1, -1))
    lax.fori_loop(0, PAIRS, back_terms, 0)
    lax.fori_loop(0, PAIRS, read_terms, 0)
    ph, pl_ = halves(pair_buf[...])
    gwr_ref[TOK : 2 * TOK] += dot(ph, w_ref[...]) + dot(pl_, w_ref[...])
    th, tl = halves(pair_buf[...].T)
    gwr_ref[0:TOK] += dot(th, r_ref[...]) + dot(tl, r_ref[...])
    spread(1, bwd_in)

    row8 = lax.broadcasted_iota(jnp.int32, (8, HD), 0)
    pick = jnp.where((lane8 < 64) == (row8 == 0), 1.0, 0.0)
    pick = jnp.where(row8 < 2, pick, 0.0).astype(BF16)

    def finish(t, carry):
        at = pl.ds(pl.multiple_of(t * HD, HD), HD)
        arriving = jnp.concatenate([bwd_in[0, t], bwd_in[1, t]], axis=0)
        sib = bwd_sibling[t]
        sib_state = jnp.concatenate([sib[0, 0:64], sib[1, 0:64]], axis=0)
        arriving = jnp.where(
            core == 0, arriving * jnp.exp(sib[0, 64:65]) + sib_state, arriving
        )
        ah, al = halves(arriving)
        x = x_ref[:, at].astype(F32)
        scale = in_scale[:, at]
        grad = back[:, at] + scale * (dot(w_ref[...], ah) + dot(w_ref[...], al))
        gi_ref[:, at] = grad
        gh, gl = halves(x * grad)
        sums = dot_nt(pick, gh) + dot_nt(pick, gl)
        gls_ref[t] = sums[0:2]
        gwr_ref[0:TOK] += three(dot_nt, x * scale, arriving)
        return carry

    lax.fori_loop(0, PAIRS, finish, 0)

    for copy in started:
        copy.wait_send()


def reduce_kernel(g_ref, gw_ref, gr_ref, got, part, whole, send, recv, send2, recv2):
    me = lax.axis_index("tp")
    depth = 2 * TOK // TP
    barrier = pltpu.get_barrier_semaphore()
    for hop in range(1, TP):
        pl.semaphore_signal(
            barrier, inc=1, device_id={"tp": lax.rem(me + hop, TP)}, device_id_type=MESH
        )
    pl.semaphore_wait(barrier, TP - 1)
    copies = []
    for hop in range(1, TP):
        to = lax.rem(me + hop, TP)
        copies.append(
            remote(
                g_ref.at[pl.ds(pl.multiple_of(to * depth, depth), depth)],
                got.at[me],
                send.at[hop],
                recv.at[me],
                "tp",
                to,
            )
        )
        copies[-1].start()
    got[me] = g_ref[pl.ds(pl.multiple_of(me * depth, depth), depth)]
    for hop in range(1, TP):
        source = lax.rem(me + hop, TP)
        remote(got.at[source], got.at[source], send.at[0], recv.at[source], "tp", source).wait_recv()
    acc = got[0]
    for i in range(1, TP):
        acc = acc + got[i]
    part[...] = acc
    for hop in range(1, TP):
        to = lax.rem(me + hop, TP)
        copies.append(
            remote(part, whole.at[me], send2.at[hop], recv2.at[me], "tp", to)
        )
        copies[-1].start()
    whole[me] = acc
    for hop in range(1, TP):
        source = lax.rem(me + hop, TP)
        remote(
            whole.at[source], whole.at[source], send2.at[0], recv2.at[source], "tp", source
        ).wait_recv()
    for i in range(TP // 2):
        gw_ref[i * depth : (i + 1) * depth] = whole[i]
        gr_ref[i * depth : (i + 1) * depth] = whole[TP // 2 + i]
    for copy in copies:
        copy.wait_send()


def vmem():
    return pl.BlockSpec(memory_space=pltpu.VMEM)


def on_device(
    query_rows, key_rows, value_rows, mixer_input, write_rows, read_rows, log_step, log_decay
):
    dma = pltpu.SemaphoreType.DMA
    packet = (PAIRS, 2, 72, HD)
    exchange = [
        pltpu.VMEM(packet, F32),
        pltpu.VMEM(packet, F32),
        pltpu.VMEM((PAIRS, 72, HD), F32),
        pltpu.VMEM((CHIPS, 72, HD), F32),
        pltpu.VMEM((CHIPS, 64, HD), F32),
        pltpu.VMEM((2, PAIRS, 64, HD), F32),
    ]
    grad_input, sums, grad_step = pl.pallas_call(
        main_kernel,
        out_shape=(
            jax.ShapeDtypeStruct((TOK, PAIRS * HD), F32),
            jax.ShapeDtypeStruct((2 * TOK, HD), F32),
            jax.ShapeDtypeStruct((PAIRS, 2, TOK), F32),
        ),
        in_specs=[vmem()] * 8,
        out_specs=(vmem(),) * 3,
        scratch_shapes=[
            pltpu.VMEM((SEQ, TOK, HD), BF16),
            pltpu.VMEM((SEQ, TOK, HD), BF16),
            pltpu.VMEM((SEQ, 8 * TOK, TOK), F32),
            pltpu.VMEM((8 * TOK, HD), F32),
            pltpu.VMEM((2 * TOK, HD), F32),
            pltpu.VMEM((2 * TOK, HD), F32),
            pltpu.VMEM((16, TOK, TOK), F32),
            pltpu.VMEM((16, TOK, TOK), BF16),
            pltpu.VMEM((16, TOK, TOK), BF16),
            pltpu.VMEM((TOK, PAIRS * HD), F32),
            pltpu.VMEM((TOK, PAIRS * HD), F32),
            pltpu.VMEM((TOK, PAIRS * HD), F32),
            pltpu.VMEM((TOK, PAIRS * HD), F32),
            pltpu.VMEM((HD, TOK), BF16),
            pltpu.VMEM((HD, TOK), BF16),
            pltpu.VMEM((TOK, TOK), F32),
            pltpu.VMEM((PAIRS, 8, HD), F32),
            *exchange,
            pltpu.VMEM((PAIRS, HD, HD), F32),
            *exchange,
            dma((16,)),
            dma((SEQ,)),
            dma((16,)),
            dma((SEQ,)),
            dma((4,)),
            dma((4,)),
            dma((2, CHIPS)),
            dma((2, CHIPS)),
            dma((2, CHIPS)),
            dma((2, CHIPS)),
        ],
        compiler_params=pltpu.CompilerParams(
            collective_id=0, has_side_effects=True, vmem_limit_bytes=60 * 1024 * 1024
        ),
        name="distill",
    )(query_rows, key_rows, value_rows, mixer_input, write_rows, read_rows, log_step, log_decay)
    depth = 2 * TOK // TP
    grad_write, grad_read = pl.pallas_call(
        reduce_kernel,
        out_shape=(jax.ShapeDtypeStruct((TOK, HD), F32),) * 2,
        in_specs=[vmem()],
        out_specs=(vmem(),) * 2,
        scratch_shapes=[
            pltpu.VMEM((TP, depth, HD), F32),
            pltpu.VMEM((depth, HD), F32),
            pltpu.VMEM((TP, depth, HD), F32),
            dma((TP,)),
            dma((TP,)),
            dma((TP,)),
            dma((TP,)),
        ],
        compiler_params=pltpu.CompilerParams(collective_id=1, has_side_effects=True),
        name="share",
    )(sums)
    return grad_input, grad_write, grad_read, grad_step.reshape(2 * PAIRS, TOK)


def solution(mesh):
    in_specs = (
        P("seq", "tp"),
        P("seq", "tp"),
        P("seq", "tp"),
        P("seq", "tp"),
        P("seq", None),
        P("seq", None),
        P("tp", "seq"),
        P("tp", "seq"),
    )
    out_specs = (P("seq", "tp"), P("seq", None), P("seq", None), P("tp", "seq"))
    return jax.shard_map(
        on_device, mesh=mesh, in_specs=in_specs, out_specs=out_specs, check_vma=False
    )
```

```python
import functools
import math

import jax
import jax.numpy as jnp
from jax import lax
from jax.experimental import pallas as pl
from jax.experimental.pallas import tpu as pltpu
from jax.sharding import PartitionSpec as P

MESH = pl.DeviceIdType.MESH
F32, BF16 = jnp.float32, jnp.bfloat16
TOK = 256
HD = 128
LOW = -1e30
SEQ = 16
CHIPS = 8
PAIRS = 8
TP = 8
SCALE = math.log2(math.e) / math.sqrt(HD)


def dot(a, b):
    return jnp.dot(a, b, preferred_element_type=F32)


def dot_nt(a, b):
    return lax.dot_general(a, b, (((1,), (1,)), ((), ())), preferred_element_type=F32)


def halves(a):
    high = a.astype(BF16)
    return high, (a - high.astype(F32)).astype(BF16)


def three(op, a, b):
    (ah, al), (bh, bl) = halves(a), halves(b)
    return op(ah, bh) + op(al, bh) + op(ah, bl)


def remote(src, dst, send_sem, recv_sem, axis, index):
    return pltpu.make_async_remote_copy(
        src_ref=src,
        dst_ref=dst,
        send_sem=send_sem,
        recv_sem=recv_sem,
        device_id={axis: index},
        device_id_type=MESH,
    )


def main_kernel(
    q_hbm,
    k_hbm,
    v_hbm,
    x_hbm,
    w_hbm,
    r_hbm,
    ls_hbm,
    ld_hbm,
    gi_hbm,
    gw_ref,
    gr_ref,
    gls_ref,
    q_ref,
    x_ref,
    w_ref,
    r_ref,
    ls_ref,
    ld_ref,
    keys,
    values,
    scores,
    peak,
    total,
    mixed,
    taught,
    decay_buf,
    mix_high,
    mix_low,
    from_start,
    in_scale,
    local_y,
    back,
    wt_buf,
    rt_buf,
    pair_buf,
    sums,
    lane_decay,
    fwd_local,
    fwd_sibling,
    fwd_chip,
    fwd_got,
    fwd_out,
    fwd_in,
    state_in,
    bwd_local,
    bwd_sibling,
    bwd_chip,
    bwd_got,
    bwd_out,
    bwd_in,
    early,
    early_got,
    part,
    read_all,
    late,
    late_got,
    write_part,
    write_all,
    in_sem,
    out_sem,
    key_send,
    key_recv,
    value_send,
    value_recv,
    sib_send,
    sib_recv,
    leg_send,
    leg_recv,
    ret_send,
    ret_recv,
    tp_send,
    tp_recv,
):
    me = lax.axis_index("seq")
    tp = lax.axis_index("tp")
    core = lax.rem(me, 2)
    chip = me // 2
    plane = lax.rem(chip, 2)
    row = me // 4
    sibling = me + 1 - 2 * core
    partner = me + 2 - 4 * plane
    above = lax.rem(me + 4, SEQ)
    below = lax.rem(me + 12, SEQ)
    far = lax.rem(me + 8, SEQ)
    above_p, below_p = lax.rem(partner + 4, SEQ), lax.rem(partner + 12, SEQ)
    far_p = lax.rem(partner + 8, SEQ)
    started = []

    barrier = pltpu.get_barrier_semaphore()
    for hop in range(1, SEQ):
        pl.semaphore_signal(
            barrier,
            inc=1,
            device_id={"seq": lax.rem(me + hop, SEQ)},
            device_id_type=MESH,
        )
    for hop in range(1, TP):
        pl.semaphore_signal(
            barrier,
            inc=1,
            device_id={"tp": lax.rem(tp + hop, TP)},
            device_id_type=MESH,
        )
    loads = [
        pltpu.make_async_copy(src, dst, in_sem.at[n])
        for n, (src, dst) in enumerate(
            (
                (k_hbm, keys.at[me]),
                (v_hbm, values.at[me]),
                (ld_hbm, ld_ref),
                (ls_hbm, ls_ref),
                (w_hbm, w_ref),
                (x_hbm, x_ref),
                (r_hbm, r_ref),
                (q_hbm, q_ref),
            )
        )
    ]
    for load in loads:
        load.start()

    def begin(copy):
        copy.start()
        started.append(copy)

    count = [0, 0]

    def pass_on(kind, index, *targets):
        store, send, recv = ((keys, key_send, key_recv), (values, value_send, value_recv))[kind]
        for target in targets:
            n = count[kind]
            count[kind] += 1
            begin(remote(store.at[index], store.at[index], send.at[n], recv.at[index], "seq", target))

    def arrived(kind, index):
        store, send, recv = ((keys, key_send, key_recv), (values, value_send, value_recv))[kind]
        remote(
            store.at[index], store.at[index], send.at[0], recv.at[index], "seq", sibling
        ).wait_recv()

    loads[0].wait()
    loads[1].wait()
    pl.semaphore_wait(barrier, SEQ + TP - 2)
    for kind in range(2):
        pass_on(kind, me, partner, above, below, sibling)

    def relay_one(kind):
        arrived(kind, partner)
        pass_on(kind, partner, above, below, sibling)
        arrived(kind, below)
        pass_on(kind, below, above, sibling)

    def relay_two(kind):
        arrived(kind, above_p)
        pass_on(kind, above_p, below, sibling)
        for index in (above, below_p):
            arrived(kind, index)
            pass_on(kind, index, sibling)

    def relay_three(kind):
        for index in (far, far_p):
            arrived(kind, index)
            pass_on(kind, index, sibling)

    rows = lax.broadcasted_iota(jnp.int32, (TOK, TOK), 0)
    cols = lax.broadcasted_iota(jnp.int32, (TOK, TOK), 1)
    causal = rows >= cols
    upper = jnp.where(rows <= cols, 1.0, 0.0).astype(BF16)
    for load in loads[2:6]:
        load.wait()
    log_decay = ld_ref[...]
    d1 = log_decay.astype(BF16)
    rest = log_decay - d1.astype(F32)
    d2 = rest.astype(BF16)
    d3 = (rest - d2.astype(F32)).astype(BF16)
    cum = dot(d1, upper) + dot(d2, upper) + dot(d3, upper)
    end = cum[:, TOK - 1 : TOK]
    row_term = ls_ref[...] - cum
    log_in = row_term + end
    columns = jnp.concatenate([cum, log_in, jnp.zeros((96, TOK), F32)], axis=0).T
    lane = lax.broadcasted_iota(jnp.int32, (TOK, HD), 1)
    first = lane < 64
    lane8 = lax.broadcasted_iota(jnp.int32, (8, HD), 1)
    wt_buf[...] = w_ref[...].T
    for t in range(PAIRS):
        a, b = 2 * t, 2 * t + 1
        at = slice(t * HD, (t + 1) * HD)
        from_start[:, at] = jnp.exp(
            jnp.where(first, columns[:, a : a + 1], columns[:, b : b + 1])
        )
        scale = jnp.exp(
            jnp.where(first, columns[:, 16 + a : 17 + a], columns[:, 16 + b : 17 + b])
        )
        in_scale[:, at] = scale
        tile = jnp.where(lane8 < 64, end[a : a + 1, :], end[b : b + 1, :])
        lane_decay[t] = tile
        high, low = halves(x_ref[:, at].astype(F32) * scale)
        state = dot(wt_buf[...], high) + dot(wt_buf[...], low)
        for half in range(2):
            fwd_local[t, half, 0:64] = state[half * 64 : (half + 1) * 64]
            fwd_local[t, half, 64:72] = tile
    begin(remote(fwd_local, fwd_sibling, sib_send.at[0], sib_recv.at[0], "seq", sibling))
    loads[6].wait()
    rt_buf[...] = r_ref[...].T
    inner = dot_nt(r_ref[...], w_ref[...])
    relay_one(0)

    def build(h):
        gap = columns[:, h : h + 1] + row_term[h : h + 1, :]
        decay = jnp.where(causal, jnp.exp(gap), 0.0)
        decay_buf[h] = decay
        high, low = halves(decay * inner)
        mix_high[h] = high
        mix_low[h] = low

    def chip_state(t, local, sib, out, early_first):
        mine, other = local[t, core], sib[t, core]
        early_core = jnp.where(core == 0, mine, other)
        late_core = jnp.where(core == 0, other, mine)
        if not early_first:
            early_core, late_core = late_core, early_core
        out[t, 0:64] = early_core[0:64] * jnp.exp(late_core[64:65]) + late_core[0:64]
        out[t, 64:72] = early_core[64:72] + late_core[64:72]

    def leg(stage, t, chip_buf, got):
        return remote(
            chip_buf.at[t],
            got.at[chip],
            leg_send.at[stage, t],
            leg_recv.at[stage, chip],
            "seq",
            2 * t + core,
        )

    def send_leg(stage, t, chip_buf, got):
        @pl.when(chip != t)
        def _():
            leg(stage, t, chip_buf, got).start()

        @pl.when(chip == t)
        def _():
            got[t] = chip_buf[t]

    def scan_leg(stage, got, out, into, order):
        for hop in range(1, CHIPS):
            source = lax.rem(chip + hop, CHIPS)
            remote(
                got.at[source],
                got.at[source],
                leg_send.at[stage, 0],
                leg_recv.at[stage, source],
                "seq",
                sibling,
            ).wait_recv()
        running = jnp.zeros((64, HD), F32)
        for i in order:
            out[i] = running
            running = running * jnp.exp(got[i, 64:65]) + got[i, 0:64]
        into[core, chip] = out[chip]
        for hop in range(1, CHIPS):
            target = lax.rem(chip + hop, CHIPS)
            begin(
                remote(
                    out.at[target],
                    into.at[core, chip],
                    ret_send.at[stage, hop],
                    ret_recv.at[stage, chip],
                    "seq",
                    2 * target + core,
                )
            )

    def spread(stage, into):
        for hop in range(1, CHIPS):
            source = lax.rem(chip + hop, CHIPS)
            remote(
                into.at[core, source],
                into.at[core, source],
                ret_send.at[stage, 0],
                ret_recv.at[stage, source],
                "seq",
                sibling,
            ).wait_recv()
        begin(
            remote(
                into.at[core],
                into.at[core],
                sib_send.at[1 + stage],
                sib_recv.at[1 + stage],
                "seq",
                sibling,
            )
        )

    def spread_wait(stage, into):
        remote(
            into.at[1 - core],
            into.at[1 - core],
            sib_send.at[1 + stage],
            sib_recv.at[1 + stage],
            "seq",
            sibling,
        ).wait_recv()

    for h in range(8):
        build(h)
    relay_one(1)
    relay_two(0)

    loads[7].wait()
    peak[...] = jnp.full(peak.shape, LOW, F32)

    def score_block(b, mask):
        kt = keys[b].T
        for h in range(8):
            at = slice(h * TOK, (h + 1) * TOK)
            s = dot(q_ref[:, h * HD : (h + 1) * HD], kt) * SCALE
            if mask:
                s = jnp.where(causal, s, LOW)
            scores[b, at] = s
            peak[at] = jnp.maximum(peak[at], jnp.maximum(s[:, :HD], s[:, HD:]))

    def score_row(shift, low):
        def step(i, carry):
            flip = lax.rem(i, 2)
            b = (
                lax.rem(row + shift, 4) * 4
                + lax.rem(plane + i // 2, 2) * 2
                + lax.rem(core + flip, 2)
            )

            @pl.when(flip == 1)
            def _():
                arrived(0, b)

            @pl.when(b < me)
            def _():
                score_block(b, False)

            return carry

        lax.fori_loop(low, 4, step, 0)

    score_block(me, True)

    @pl.when(core == 0)
    def _():
        scores[me + 1] = jnp.full((8 * TOK, TOK), LOW, F32)

    for h in range(8, 16):
        build(h)
    score_row(0, 1)
    relay_two(1)
    relay_three(0)
    remote(
        fwd_sibling, fwd_sibling, sib_send.at[0], sib_recv.at[0], "seq", sibling
    ).wait_recv()
    for t in range(PAIRS):
        chip_state(t, fwd_local, fwd_sibling, fwd_chip, True)
        send_leg(0, t, fwd_chip, fwd_got)
    score_row(3, 0)
    score_row(1, 0)
    relay_three(1)

    def make_y(t, carry):
        at = pl.ds(pl.multiple_of(t * HD, HD), HD)
        x = x_ref[:, at]
        xa = jnp.where(first, x, jnp.zeros_like(x))
        xb = jnp.where(first, jnp.zeros_like(x), x)
        local_y[:, at] = (
            dot(mix_high[2 * t], xa)
            + dot(mix_low[2 * t], xa)
            + dot(mix_high[2 * t + 1], xb)
            + dot(mix_low[2 * t + 1], xb)
        )
        return carry

    lax.fori_loop(0, PAIRS, make_y, 0)
    score_row(2, 0)
    scan_leg(0, fwd_got, fwd_out, fwd_in, range(CHIPS))
    for index in (me, partner, above, below, above_p, below_p, far, far_p):
        arrived(1, index + 1 - 2 * core)

    def weigh(g):
        at2 = slice(g * 2 * TOK, (g + 1) * 2 * TOK)
        top = jnp.max(peak[at2], axis=1, keepdims=True)
        total[...] = jnp.zeros(total.shape, F32)
        mixed[...] = jnp.zeros(mixed.shape, F32)

        def chunk(n, carry):
            for b in (2 * n, 2 * n + 1):
                weights = jnp.exp2(scores[b, at2] - top)
                total[...] += weights[:, :HD] + weights[:, HD:]
                mixed[...] += dot(weights.astype(BF16), values[b])
            return carry

        lax.fori_loop(0, chip + 1, chunk, 0)
        ratio = mixed[...] / jnp.sum(total[...], axis=1, keepdims=True)
        taught[at2] = ratio.astype(BF16)

    def meet(g):
        for t in (2 * g, 2 * g + 1):
            at = slice(t * HD, (t + 1) * HD)
            entering = jnp.concatenate([fwd_in[0, t], fwd_in[1, t]], axis=0)
            sib = fwd_sibling[t]
            sib_state = jnp.concatenate([sib[0, 0:64], sib[1, 0:64]], axis=0)
            entering = jnp.where(
                core == 1, entering * jnp.exp(sib[0, 64:65]) + sib_state, entering
            )
            state_in[t] = entering
            sh, sl = halves(entering)
            starts = from_start[:, at]
            carried = (dot(r_ref[...], sh) + dot(r_ref[...], sl)) * starts
            residual = local_y[:, at] + carried - taught[t * TOK : (t + 1) * TOK].astype(F32)
            local_y[:, at] = residual
            wh, wl = halves(residual * starts)
            adjoint = dot(rt_buf[...], wh) + dot(rt_buf[...], wl)
            for half in range(2):
                bwd_local[t, half, 0:64] = adjoint[half * 64 : (half + 1) * 64]
                bwd_local[t, half, 64:72] = lane_decay[t]
        two = pl.ds(2 * g, 2)
        begin(
            remote(
                bwd_local.at[two],
                bwd_sibling.at[two],
                sib_send.at[3 + g],
                sib_recv.at[3 + g],
                "seq",
                sibling,
            )
        )

    def hand_over(g):
        two = pl.ds(2 * g, 2)
        remote(
            bwd_sibling.at[two],
            bwd_sibling.at[two],
            sib_send.at[3 + g],
            sib_recv.at[3 + g],
            "seq",
            sibling,
        ).wait_recv()
        for t in (2 * g, 2 * g + 1):
            chip_state(t, bwd_local, bwd_sibling, bwd_chip, False)
            send_leg(1, t, bwd_chip, bwd_got)

    def local_terms(t, carry):
        at = pl.ds(pl.multiple_of(t * HD, HD), HD)
        residual = local_y[:, at]
        xt = x_ref[:, at].T
        for side, own in ((0, first), (1, ~first)):
            rh, rl = halves(jnp.where(own, residual, 0.0))
            pair_buf[...] += decay_buf[2 * t + side] * (dot(rh, xt) + dot(rl, xt))
        return carry

    def back_terms(t, carry):
        at = pl.ds(pl.multiple_of(t * HD, HD), HD)
        residual_t = local_y[:, at].T
        rh, rl = halves(residual_t)
        pieces = []
        for side in range(2):
            own = slice(side * 64, (side + 1) * 64)
            both = jnp.concatenate([rh[own], rl[own]], axis=0)
            product = dot(both, mix_high[2 * t + side])
            pieces.append(product[0:64] + product[64:128] + dot(rh[own], mix_low[2 * t + side]))
        back[:, at] = jnp.concatenate(pieces, axis=0).T
        return carry

    def read_terms(t, carry):
        at = pl.ds(pl.multiple_of(t * HD, HD), HD)
        weighted = local_y[:, at] * from_start[:, at]
        sums[...] += three(dot_nt, weighted, state_in[t])
        return carry

    pair_buf[...] = jnp.zeros(pair_buf.shape, F32)
    sums[...] = jnp.zeros(sums.shape, F32)
    weigh(0)
    weigh(1)
    spread(0, fwd_in)
    weigh(2)
    spread_wait(0, fwd_in)
    meet(0)
    meet(1)
    hand_over(0)
    meet(2)
    hand_over(1)
    weigh(3)
    hand_over(2)
    meet(3)
    lax.fori_loop(0, 4, local_terms, 0)
    hand_over(3)
    lax.fori_loop(4, PAIRS, local_terms, 0)
    lax.fori_loop(0, PAIRS, read_terms, 0)
    ph, pw = halves(pair_buf[...])
    grad_read = sums[...] + dot(ph, w_ref[...]) + dot(pw, w_ref[...])
    th, tl = halves(pair_buf[...].T)
    grad_write = dot(th, r_ref[...]) + dot(tl, r_ref[...])
    for i in range(TP):
        early[i, 0:32] = grad_write[i * 32 : (i + 1) * 32]
        early[i, 32:64] = grad_read[i * 32 : (i + 1) * 32]

    def scatter(stage, source, got):
        got[tp] = source[tp]
        for hop in range(1, TP):
            to = lax.rem(tp + hop, TP)
            begin(
                remote(
                    source.at[to], got.at[tp], tp_send.at[stage, hop], tp_recv.at[stage, tp], "tp", to
                )
            )

    def gather(stage, source, got):
        got[tp] = source[...]
        for hop in range(1, TP):
            to = lax.rem(tp + hop, TP)
            begin(
                remote(source, got.at[tp], tp_send.at[stage, hop], tp_recv.at[stage, tp], "tp", to)
            )

    def collect(stage, got):
        for hop in range(1, TP):
            source = lax.rem(tp + hop, TP)
            remote(
                got.at[source],
                got.at[source],
                tp_send.at[stage, 0],
                tp_recv.at[stage, source],
                "tp",
                source,
            ).wait_recv()

    scatter(0, early, early_got)
    scan_leg(1, bwd_got, bwd_out, bwd_in, range(CHIPS - 1, -1, -1))
    lax.fori_loop(0, PAIRS, back_terms, 0)
    collect(0, early_got)
    acc = early_got[0]
    for i in range(1, TP):
        acc = acc + early_got[i]
    part[...] = acc
    gather(1, part.at[32:64], read_all)
    spread(1, bwd_in)
    spread_wait(1, bwd_in)

    def carry_terms(t, carry):
        at = pl.ds(pl.multiple_of(t * HD, HD), HD)
        arriving = jnp.concatenate([bwd_in[0, t], bwd_in[1, t]], axis=0)
        sib = bwd_sibling[t]
        sib_state = jnp.concatenate([sib[0, 0:64], sib[1, 0:64]], axis=0)
        arriving = jnp.where(
            core == 0, arriving * jnp.exp(sib[0, 64:65]) + sib_state, arriving
        )
        state_in[t] = arriving
        sums[...] += three(dot_nt, x_ref[:, at].astype(F32) * in_scale[:, at], arriving)
        return carry

    sums[...] = jnp.zeros(sums.shape, F32)
    lax.fori_loop(0, PAIRS, carry_terms, 0)
    for i in range(TP):
        late[i] = sums[i * 32 : (i + 1) * 32]
    scatter(2, late, late_got)

    row16 = lax.broadcasted_iota(jnp.int32, (16, HD), 0)
    lane16 = lax.broadcasted_iota(jnp.int32, (16, HD), 1)
    gls_ref[...] = jnp.zeros(gls_ref.shape, F32)

    def store_of(t):
        at = pl.ds(pl.multiple_of(t * HD, HD), HD)
        return pltpu.make_async_copy(back.at[:, at], gi_hbm.at[:, at], out_sem.at[t])

    def finish(t, carry):
        at = pl.ds(pl.multiple_of(t * HD, HD), HD)
        ah, al = halves(state_in[t])
        grad = back[:, at] + in_scale[:, at] * (dot(w_ref[...], ah) + dot(w_ref[...], al))
        back[:, at] = grad
        store_of(t).start()
        gh, gl = halves(x_ref[:, at].astype(F32) * grad)
        pick = jnp.where(row16 == 2 * t + lane16 // 64, 1.0, 0.0).astype(BF16)
        gls_ref[...] += dot_nt(pick, gh) + dot_nt(pick, gl)
        return carry

    lax.fori_loop(0, PAIRS, finish, 0)
    collect(1, read_all)
    for i in range(TP):
        gr_ref[i * 32 : (i + 1) * 32] = read_all[i]
    collect(2, late_got)
    acc = part[0:32]
    for i in range(TP):
        acc = acc + late_got[i]
    write_part[...] = acc
    gather(3, write_part, write_all)
    for t in range(PAIRS):
        store_of(t).wait()
    for copy in started:
        copy.wait_send()
    for t in range(PAIRS):

        @pl.when(chip != t)
        def _():
            leg(0, t, fwd_chip, fwd_got).wait_send()
            leg(1, t, bwd_chip, bwd_got).wait_send()

    collect(3, write_all)
    for i in range(TP):
        gw_ref[i * 32 : (i + 1) * 32] = write_all[i]


def on_device(
    query_rows, key_rows, value_rows, mixer_input, write_rows, read_rows, log_step, log_decay
):
    dma = pltpu.SemaphoreType.DMA
    packet = (PAIRS, 2, 72, HD)
    exchange = [
        pltpu.VMEM(packet, F32),
        pltpu.VMEM(packet, F32),
        pltpu.VMEM((PAIRS, 72, HD), F32),
        pltpu.VMEM((CHIPS, 72, HD), F32),
        pltpu.VMEM((CHIPS, 64, HD), F32),
        pltpu.VMEM((2, PAIRS, 64, HD), F32),
    ]
    whole = pl.BlockSpec(memory_space=pl.ANY)
    vmem = pl.BlockSpec(memory_space=pltpu.VMEM)
    wide = (TOK, PAIRS * HD)
    share = (TP, 32, HD)
    return pl.pallas_call(
        main_kernel,
        out_shape=(
            jax.ShapeDtypeStruct(wide, F32),
            jax.ShapeDtypeStruct((TOK, HD), F32),
            jax.ShapeDtypeStruct((TOK, HD), F32),
            jax.ShapeDtypeStruct((2 * PAIRS, TOK), F32),
        ),
        in_specs=[whole] * 8,
        out_specs=(whole, vmem, vmem, vmem),
        scratch_shapes=[
            pltpu.VMEM(wide, BF16),
            pltpu.VMEM(wide, BF16),
            pltpu.VMEM((TOK, HD), BF16),
            pltpu.VMEM((TOK, HD), BF16),
            pltpu.VMEM((2 * PAIRS, TOK), F32),
            pltpu.VMEM((2 * PAIRS, TOK), F32),
            pltpu.VMEM((SEQ, TOK, HD), BF16),
            pltpu.VMEM((SEQ, TOK, HD), BF16),
            pltpu.VMEM((SEQ, 8 * TOK, TOK), F32),
            pltpu.VMEM((8 * TOK, HD), F32),
            pltpu.VMEM((2 * TOK, HD), F32),
            pltpu.VMEM((2 * TOK, HD), F32),
            pltpu.VMEM((8 * TOK, HD), BF16),
            pltpu.VMEM((16, TOK, TOK), F32),
            pltpu.VMEM((16, TOK, TOK), BF16),
            pltpu.VMEM((16, TOK, TOK), BF16),
            pltpu.VMEM(wide, F32),
            pltpu.VMEM(wide, F32),
            pltpu.VMEM(wide, F32),
            pltpu.VMEM(wide, F32),
            pltpu.VMEM((HD, TOK), BF16),
            pltpu.VMEM((HD, TOK), BF16),
            pltpu.VMEM((TOK, TOK), F32),
            pltpu.VMEM((TOK, HD), F32),
            pltpu.VMEM((PAIRS, 8, HD), F32),
            *exchange,
            pltpu.VMEM((PAIRS, HD, HD), F32),
            *exchange,
            pltpu.VMEM((TP, 64, HD), F32),
            pltpu.VMEM((TP, 64, HD), F32),
            pltpu.VMEM((64, HD), F32),
            pltpu.VMEM(share, F32),
            pltpu.VMEM(share, F32),
            pltpu.VMEM(share, F32),
            pltpu.VMEM((32, HD), F32),
            pltpu.VMEM(share, F32),
            dma((8,)),
            dma((PAIRS,)),
            dma((16,)),
            dma((SEQ,)),
            dma((16,)),
            dma((SEQ,)),
            dma((8,)),
            dma((8,)),
            dma((2, CHIPS)),
            dma((2, CHIPS)),
            dma((2, CHIPS)),
            dma((2, CHIPS)),
            dma((4, TP)),
            dma((4, TP)),
        ],
        compiler_params=pltpu.CompilerParams(
            collective_id=0, has_side_effects=True, vmem_limit_bytes=61 * 1024 * 1024
        ),
        name="distill",
    )(query_rows, key_rows, value_rows, mixer_input, write_rows, read_rows, log_step, log_decay)


def solution(mesh):
    in_specs = (
        P("seq", "tp"),
        P("seq", "tp"),
        P("seq", "tp"),
        P("seq", "tp"),
        P("seq", None),
        P("seq", None),
        P("tp", "seq"),
        P("tp", "seq"),
    )
    out_specs = (P("seq", "tp"), P("seq", None), P("seq", None), P("tp", "seq"))
    return jax.shard_map(
        on_device, mesh=mesh, in_specs=in_specs, out_specs=out_specs, check_vma=False
    )
```

```python
import functools
import math

import jax
import jax.numpy as jnp
from jax import lax
from jax.experimental import pallas as pl
from jax.experimental.pallas import tpu as pltpu
from jax.sharding import PartitionSpec as P

MESH = pl.DeviceIdType.MESH
F32, BF16 = jnp.float32, jnp.bfloat16
TOK = 256
HD = 128
LOW = -1e30
SEQ = 16
CHIPS = 8
PAIRS = 8
TP = 8
SCALE = math.log2(math.e) / math.sqrt(HD)


def dot(a, b):
    return jnp.dot(a, b, preferred_element_type=F32)


def dot_nt(a, b):
    return lax.dot_general(a, b, (((1,), (1,)), ((), ())), preferred_element_type=F32)


def halves(a):
    high = a.astype(BF16)
    return high, (a - high.astype(F32)).astype(BF16)


def three(op, a, b):
    (ah, al), (bh, bl) = halves(a), halves(b)
    return op(ah, bh) + op(al, bh) + op(ah, bl)


def remote(src, dst, send_sem, recv_sem, axis, index):
    return pltpu.make_async_remote_copy(
        src_ref=src,
        dst_ref=dst,
        send_sem=send_sem,
        recv_sem=recv_sem,
        device_id={axis: index},
        device_id_type=MESH,
    )


def main_kernel(
    q_hbm,
    k_hbm,
    v_hbm,
    x_hbm,
    w_hbm,
    r_hbm,
    ls_hbm,
    ld_hbm,
    back,
    gw_ref,
    gr_ref,
    gls_ref,
    q_ref,
    x_ref,
    w_ref,
    r_ref,
    ls_ref,
    ld_ref,
    keys,
    values,
    scores,
    peak,
    total,
    mixed,
    taught,
    decay_buf,
    mix_high,
    mix_low,
    from_start,
    in_scale,
    local_y,
    wt_buf,
    rt_buf,
    pair_buf,
    sums,
    lane_decay,
    fwd_local,
    fwd_sibling,
    fwd_chip,
    fwd_got,
    fwd_out,
    fwd_in,
    state_in,
    bwd_local,
    bwd_sibling,
    bwd_chip,
    bwd_got,
    bwd_out,
    bwd_in,
    early,
    early_got,
    part,
    read_all,
    late,
    late_got,
    write_part,
    write_all,
    in_sem,
    key_send,
    key_recv,
    value_send,
    value_recv,
    sib_send,
    sib_recv,
    leg_send,
    leg_recv,
    ret_send,
    ret_recv,
    tp_send,
    tp_recv,
):
    me = lax.axis_index("seq")
    tp = lax.axis_index("tp")
    core = lax.rem(me, 2)
    chip = me // 2
    plane = lax.rem(chip, 2)
    row = me // 4
    sibling = me + 1 - 2 * core
    partner = me + 2 - 4 * plane
    above = lax.rem(me + 4, SEQ)
    below = lax.rem(me + 12, SEQ)
    far = lax.rem(me + 8, SEQ)
    above_p, below_p = lax.rem(partner + 4, SEQ), lax.rem(partner + 12, SEQ)
    far_p = lax.rem(partner + 8, SEQ)
    started = []

    barrier = pltpu.get_barrier_semaphore()
    for hop in range(1, SEQ):
        pl.semaphore_signal(
            barrier,
            inc=1,
            device_id={"seq": lax.rem(me + hop, SEQ)},
            device_id_type=MESH,
        )
    for hop in range(1, TP):
        pl.semaphore_signal(
            barrier,
            inc=1,
            device_id={"tp": lax.rem(tp + hop, TP)},
            device_id_type=MESH,
        )
    loads = [
        pltpu.make_async_copy(src, dst, in_sem.at[n])
        for n, (src, dst) in enumerate(
            (
                (k_hbm, keys.at[me]),
                (v_hbm, values.at[me]),
                (ld_hbm, ld_ref),
                (ls_hbm, ls_ref),
                (w_hbm, w_ref),
                (x_hbm, x_ref),
                (r_hbm, r_ref),
                (q_hbm, q_ref),
            )
        )
    ]
    for load in loads:
        load.start()

    def begin(copy):
        copy.start()
        started.append(copy)

    count = [0, 0]

    def pass_on(kind, index, *targets):
        store, send, recv = ((keys, key_send, key_recv), (values, value_send, value_recv))[kind]
        for target in targets:
            n = count[kind]
            count[kind] += 1
            begin(remote(store.at[index], store.at[index], send.at[n], recv.at[index], "seq", target))

    def arrived(kind, index):
        store, send, recv = ((keys, key_send, key_recv), (values, value_send, value_recv))[kind]
        remote(
            store.at[index], store.at[index], send.at[0], recv.at[index], "seq", sibling
        ).wait_recv()

    loads[0].wait()
    loads[1].wait()
    pl.semaphore_wait(barrier, SEQ + TP - 2)
    for kind in range(2):
        pass_on(kind, me, partner, above, below, sibling)

    def relay_one(kind):
        arrived(kind, partner)
        pass_on(kind, partner, above, below, sibling)
        arrived(kind, below)
        pass_on(kind, below, above, sibling)

    def relay_two(kind):
        arrived(kind, above_p)
        pass_on(kind, above_p, below, sibling)
        for index in (above, below_p):
            arrived(kind, index)
            pass_on(kind, index, sibling)

    def relay_three(kind):
        for index in (far, far_p):
            arrived(kind, index)
            pass_on(kind, index, sibling)

    rows = lax.broadcasted_iota(jnp.int32, (TOK, TOK), 0)
    cols = lax.broadcasted_iota(jnp.int32, (TOK, TOK), 1)
    causal = rows >= cols
    upper = jnp.where(rows <= cols, 1.0, 0.0).astype(BF16)
    for load in loads[2:6]:
        load.wait()
    log_decay = ld_ref[...]
    d1 = log_decay.astype(BF16)
    rest = log_decay - d1.astype(F32)
    d2 = rest.astype(BF16)
    d3 = (rest - d2.astype(F32)).astype(BF16)
    cum = dot(d1, upper) + dot(d2, upper) + dot(d3, upper)
    end = cum[:, TOK - 1 : TOK]
    row_term = ls_ref[...] - cum
    log_in = row_term + end
    columns = jnp.concatenate([cum, log_in, jnp.zeros((96, TOK), F32)], axis=0).T
    lane = lax.broadcasted_iota(jnp.int32, (TOK, HD), 1)
    first = lane < 64
    lane8 = lax.broadcasted_iota(jnp.int32, (8, HD), 1)
    wt_buf[...] = w_ref[...].T
    for t in range(PAIRS):
        a, b = 2 * t, 2 * t + 1
        at = slice(t * HD, (t + 1) * HD)
        from_start[:, at] = jnp.exp(
            jnp.where(first, columns[:, a : a + 1], columns[:, b : b + 1])
        )
        scale = jnp.exp(
            jnp.where(first, columns[:, 16 + a : 17 + a], columns[:, 16 + b : 17 + b])
        )
        in_scale[:, at] = scale
        tile = jnp.where(lane8 < 64, end[a : a + 1, :], end[b : b + 1, :])
        lane_decay[t] = tile
        high, low = halves(x_ref[:, at].astype(F32) * scale)
        state = dot(wt_buf[...], high) + dot(wt_buf[...], low)
        for half in range(2):
            fwd_local[t, half, 0:64] = state[half * 64 : (half + 1) * 64]
            fwd_local[t, half, 64:72] = tile
    begin(remote(fwd_local, fwd_sibling, sib_send.at[0], sib_recv.at[0], "seq", sibling))
    loads[6].wait()
    rt_buf[...] = r_ref[...].T
    inner = dot_nt(r_ref[...], w_ref[...])
    relay_one(0)

    def build(h):
        gap = columns[:, h : h + 1] + row_term[h : h + 1, :]
        decay = jnp.where(causal, jnp.exp(gap), 0.0)
        decay_buf[h] = decay
        high, low = halves(decay * inner)
        mix_high[h] = high
        mix_low[h] = low

    def chip_state(t, local, sib, out, early_first):
        mine, other = local[t, core], sib[t, core]
        early_core = jnp.where(core == 0, mine, other)
        late_core = jnp.where(core == 0, other, mine)
        if not early_first:
            early_core, late_core = late_core, early_core
        out[t, 0:64] = early_core[0:64] * jnp.exp(late_core[64:65]) + late_core[0:64]
        out[t, 64:72] = early_core[64:72] + late_core[64:72]

    def leg(stage, t, chip_buf, got):
        return remote(
            chip_buf.at[t],
            got.at[chip],
            leg_send.at[stage, t],
            leg_recv.at[stage, chip],
            "seq",
            2 * t + core,
        )

    def send_leg(stage, t, chip_buf, got):
        @pl.when(chip != t)
        def _():
            leg(stage, t, chip_buf, got).start()

        @pl.when(chip == t)
        def _():
            got[t] = chip_buf[t]

    def scan_leg(stage, got, out, into, order):
        for hop in range(1, CHIPS):
            source = lax.rem(chip + hop, CHIPS)
            remote(
                got.at[source],
                got.at[source],
                leg_send.at[stage, 0],
                leg_recv.at[stage, source],
                "seq",
                sibling,
            ).wait_recv()
        running = jnp.zeros((64, HD), F32)
        for i in order:
            out[i] = running
            running = running * jnp.exp(got[i, 64:65]) + got[i, 0:64]
        into[core, chip] = out[chip]
        for hop in range(1, CHIPS):
            target = lax.rem(chip + hop, CHIPS)
            begin(
                remote(
                    out.at[target],
                    into.at[core, chip],
                    ret_send.at[stage, hop],
                    ret_recv.at[stage, chip],
                    "seq",
                    2 * target + core,
                )
            )

    def spread(stage, into):
        for hop in range(1, CHIPS):
            source = lax.rem(chip + hop, CHIPS)
            remote(
                into.at[core, source],
                into.at[core, source],
                ret_send.at[stage, 0],
                ret_recv.at[stage, source],
                "seq",
                sibling,
            ).wait_recv()
        begin(
            remote(
                into.at[core],
                into.at[core],
                sib_send.at[1 + stage],
                sib_recv.at[1 + stage],
                "seq",
                sibling,
            )
        )

    def spread_wait(stage, into):
        remote(
            into.at[1 - core],
            into.at[1 - core],
            sib_send.at[1 + stage],
            sib_recv.at[1 + stage],
            "seq",
            sibling,
        ).wait_recv()

    remote(
        fwd_sibling, fwd_sibling, sib_send.at[0], sib_recv.at[0], "seq", sibling
    ).wait_recv()
    for t in range(PAIRS):
        chip_state(t, fwd_local, fwd_sibling, fwd_chip, True)
        send_leg(0, t, fwd_chip, fwd_got)
    for h in range(8):
        build(h)
    relay_one(1)
    relay_two(0)

    loads[7].wait()
    peak[...] = jnp.full(peak.shape, LOW, F32)

    def score_block(b, mask):
        kt = keys[b].T
        for h in range(8):
            at = slice(h * TOK, (h + 1) * TOK)
            s = dot(q_ref[:, h * HD : (h + 1) * HD], kt) * SCALE
            if mask:
                s = jnp.where(causal, s, LOW)
            scores[b, at] = s
            peak[at] = jnp.maximum(peak[at], jnp.maximum(s[:, :HD], s[:, HD:]))

    def score_other(shift):
        other = lax.rem(row + shift, 4)

        def step(i, carry):
            base = other * 4 + lax.rem(plane + i, 2) * 2
            arrived(0, base + 1 - core)

            @pl.when(other < row)
            def _():
                score_block(base, False)
                score_block(base + 1, False)

            return carry

        lax.fori_loop(0, 2, step, 0)

    def score_row(shift, low):
        def step(i, carry):
            flip = lax.rem(i, 2)
            b = (
                lax.rem(row + shift, 4) * 4
                + lax.rem(plane + i // 2, 2) * 2
                + lax.rem(core + flip, 2)
            )

            @pl.when(flip == 1)
            def _():
                arrived(0, b)

            @pl.when(b < me)
            def _():
                score_block(b, False)

            return carry

        lax.fori_loop(low, 4, step, 0)

    score_block(me, True)

    def blank(b, carry):
        scores[b] = jnp.full((8 * TOK, TOK), LOW, F32)
        return carry

    lax.fori_loop(me + 1, 4 * row + 4, blank, 0)

    for h in range(8, 16):
        build(h)
    score_row(0, 1)
    relay_two(1)
    relay_three(0)
    score_other(3)
    scan_leg(0, fwd_got, fwd_out, fwd_in, range(CHIPS))
    score_other(1)
    relay_three(1)

    def make_y(t, carry):
        at = pl.ds(pl.multiple_of(t * HD, HD), HD)
        x = x_ref[:, at]
        xa = jnp.where(first, x, jnp.zeros_like(x))
        xb = jnp.where(first, jnp.zeros_like(x), x)
        local_y[:, at] = (
            dot(mix_high[2 * t], xa)
            + dot(mix_low[2 * t], xa)
            + dot(mix_high[2 * t + 1], xb)
            + dot(mix_low[2 * t + 1], xb)
        )
        return carry

    lax.fori_loop(0, PAIRS, make_y, 0)
    score_other(2)
    for index in (me, partner, above, below, above_p, below_p, far, far_p):
        arrived(1, index + 1 - 2 * core)

    def weigh(g):
        at2 = slice(g * 2 * TOK, (g + 1) * 2 * TOK)
        top = jnp.max(peak[at2], axis=1, keepdims=True)
        total[...] = jnp.zeros(total.shape, F32)
        mixed[...] = jnp.zeros(mixed.shape, F32)

        def chunk(n, carry):
            low, folded = [], None
            for b in range(4):
                weights = jnp.exp2(scores[4 * n + b, at2] - top)
                low.append(weights.astype(BF16))
                both = weights[:, :HD] + weights[:, HD:]
                folded = both if folded is None else folded + both
            total[...] += folded
            shown = values[pl.ds(4 * n, 4)].reshape(4 * TOK, HD)
            mixed[...] += dot(jnp.concatenate(low, axis=1), shown)
            return carry

        lax.fori_loop(0, row + 1, chunk, 0)
        ratio = mixed[...] / jnp.sum(total[...], axis=1, keepdims=True)
        taught[at2] = ratio.astype(BF16)

    def meet(g):
        for t in (2 * g, 2 * g + 1):
            at = slice(t * HD, (t + 1) * HD)
            entering = jnp.concatenate([fwd_in[0, t], fwd_in[1, t]], axis=0)
            sib = fwd_sibling[t]
            sib_state = jnp.concatenate([sib[0, 0:64], sib[1, 0:64]], axis=0)
            entering = jnp.where(
                core == 1, entering * jnp.exp(sib[0, 64:65]) + sib_state, entering
            )
            state_in[t] = entering
            sh, sl = halves(entering)
            starts = from_start[:, at]
            carried = (dot(r_ref[...], sh) + dot(r_ref[...], sl)) * starts
            residual = local_y[:, at] + carried - taught[t * TOK : (t + 1) * TOK].astype(F32)
            local_y[:, at] = residual
            wh, wl = halves(residual * starts)
            adjoint = dot(rt_buf[...], wh) + dot(rt_buf[...], wl)
            for half in range(2):
                bwd_local[t, half, 0:64] = adjoint[half * 64 : (half + 1) * 64]
                bwd_local[t, half, 64:72] = lane_decay[t]
        two = pl.ds(2 * g, 2)
        begin(
            remote(
                bwd_local.at[two],
                bwd_sibling.at[two],
                sib_send.at[3 + g],
                sib_recv.at[3 + g],
                "seq",
                sibling,
            )
        )

    def hand_over(g):
        two = pl.ds(2 * g, 2)
        remote(
            bwd_sibling.at[two],
            bwd_sibling.at[two],
            sib_send.at[3 + g],
            sib_recv.at[3 + g],
            "seq",
            sibling,
        ).wait_recv()
        for t in (2 * g, 2 * g + 1):
            chip_state(t, bwd_local, bwd_sibling, bwd_chip, False)
            send_leg(1, t, bwd_chip, bwd_got)

    def local_terms(t, carry):
        at = pl.ds(pl.multiple_of(t * HD, HD), HD)
        residual = local_y[:, at]
        xt = x_ref[:, at].T
        for side, own in ((0, first), (1, ~first)):
            rh, rl = halves(jnp.where(own, residual, 0.0))
            pair_buf[...] += decay_buf[2 * t + side] * (dot(rh, xt) + dot(rl, xt))
        return carry

    def back_terms(t, carry):
        at = pl.ds(pl.multiple_of(t * HD, HD), HD)
        residual_t = local_y[:, at].T
        rh, rl = halves(residual_t)
        pieces = []
        for side in range(2):
            own = slice(side * 64, (side + 1) * 64)
            both = jnp.concatenate([rh[own], rl[own]], axis=0)
            product = dot(both, mix_high[2 * t + side])
            pieces.append(product[0:64] + product[64:128] + dot(rh[own], mix_low[2 * t + side]))
        back[:, at] = jnp.concatenate(pieces, axis=0).T
        return carry

    def read_terms(t, carry):
        at = pl.ds(pl.multiple_of(t * HD, HD), HD)
        weighted = local_y[:, at] * from_start[:, at]
        sums[...] += three(dot_nt, weighted, state_in[t])
        return carry

    pair_buf[...] = jnp.zeros(pair_buf.shape, F32)
    sums[...] = jnp.zeros(sums.shape, F32)
    weigh(0)
    weigh(1)
    spread(0, fwd_in)
    weigh(2)
    spread_wait(0, fwd_in)
    meet(0)
    meet(1)
    hand_over(0)
    meet(2)
    hand_over(1)
    weigh(3)
    hand_over(2)
    meet(3)
    lax.fori_loop(0, 4, local_terms, 0)
    hand_over(3)
    lax.fori_loop(4, PAIRS, local_terms, 0)
    lax.fori_loop(0, PAIRS, read_terms, 0)
    ph, pw = halves(pair_buf[...])
    grad_read = sums[...] + dot(ph, w_ref[...]) + dot(pw, w_ref[...])
    th, tl = halves(pair_buf[...].T)
    grad_write = dot(th, r_ref[...]) + dot(tl, r_ref[...])
    for i in range(TP):
        early[i, 0:32] = grad_write[i * 32 : (i + 1) * 32]
        early[i, 32:64] = grad_read[i * 32 : (i + 1) * 32]

    def scatter(stage, source, got):
        got[tp] = source[tp]
        for hop in range(1, TP):
            to = lax.rem(tp + hop, TP)
            begin(
                remote(
                    source.at[to], got.at[tp], tp_send.at[stage, hop], tp_recv.at[stage, tp], "tp", to
                )
            )

    def gather(stage, source, got):
        got[tp] = source[...]
        for hop in range(1, TP):
            to = lax.rem(tp + hop, TP)
            begin(
                remote(source, got.at[tp], tp_send.at[stage, hop], tp_recv.at[stage, tp], "tp", to)
            )

    def collect(stage, got):
        for hop in range(1, TP):
            source = lax.rem(tp + hop, TP)
            remote(
                got.at[source],
                got.at[source],
                tp_send.at[stage, 0],
                tp_recv.at[stage, source],
                "tp",
                source,
            ).wait_recv()

    scatter(0, early, early_got)
    scan_leg(1, bwd_got, bwd_out, bwd_in, range(CHIPS - 1, -1, -1))
    lax.fori_loop(0, PAIRS, back_terms, 0)
    collect(0, early_got)
    acc = early_got[0]
    for i in range(1, TP):
        acc = acc + early_got[i]
    part[...] = acc
    gather(1, part.at[32:64], read_all)
    spread(1, bwd_in)
    spread_wait(1, bwd_in)

    def carry_terms(t, carry):
        at = pl.ds(pl.multiple_of(t * HD, HD), HD)
        arriving = jnp.concatenate([bwd_in[0, t], bwd_in[1, t]], axis=0)
        sib = bwd_sibling[t]
        sib_state = jnp.concatenate([sib[0, 0:64], sib[1, 0:64]], axis=0)
        arriving = jnp.where(
            core == 0, arriving * jnp.exp(sib[0, 64:65]) + sib_state, arriving
        )
        state_in[t] = arriving
        sums[...] += three(dot_nt, x_ref[:, at].astype(F32) * in_scale[:, at], arriving)
        return carry

    sums[...] = jnp.zeros(sums.shape, F32)
    lax.fori_loop(0, PAIRS, carry_terms, 0)
    for i in range(TP):
        late[i] = sums[i * 32 : (i + 1) * 32]
    scatter(2, late, late_got)

    row16 = lax.broadcasted_iota(jnp.int32, (16, HD), 0)
    lane16 = lax.broadcasted_iota(jnp.int32, (16, HD), 1)
    gls_ref[...] = jnp.zeros(gls_ref.shape, F32)

    def finish(t, carry):
        at = pl.ds(pl.multiple_of(t * HD, HD), HD)
        ah, al = halves(state_in[t])
        grad = back[:, at] + in_scale[:, at] * (dot(w_ref[...], ah) + dot(w_ref[...], al))
        back[:, at] = grad
        gh, gl = halves(x_ref[:, at].astype(F32) * grad)
        pick = jnp.where(row16 == 2 * t + lane16 // 64, 1.0, 0.0).astype(BF16)
        gls_ref[...] += dot_nt(pick, gh) + dot_nt(pick, gl)
        return carry

    lax.fori_loop(0, PAIRS, finish, 0)
    collect(1, read_all)
    for i in range(TP):
        gr_ref[i * 32 : (i + 1) * 32] = read_all[i]
    collect(2, late_got)
    acc = part[0:32]
    for i in range(TP):
        acc = acc + late_got[i]
    write_part[...] = acc
    gather(3, write_part, write_all)
    for copy in started:
        copy.wait_send()
    for t in range(PAIRS):

        @pl.when(chip != t)
        def _():
            leg(0, t, fwd_chip, fwd_got).wait_send()
            leg(1, t, bwd_chip, bwd_got).wait_send()

    collect(3, write_all)
    for i in range(TP):
        gw_ref[i * 32 : (i + 1) * 32] = write_all[i]


def write_kernel(*refs):
    copies = [
        pltpu.make_async_copy(src, dst, refs[8].at[n])
        for n, (src, dst) in enumerate(zip(refs[0:4], refs[4:8]))
    ]
    for copy in copies:
        copy.start()
    for copy in copies:
        copy.wait()


def on_device(
    query_rows, key_rows, value_rows, mixer_input, write_rows, read_rows, log_step, log_decay
):
    dma = pltpu.SemaphoreType.DMA
    packet = (PAIRS, 2, 72, HD)
    exchange = [
        pltpu.VMEM(packet, F32),
        pltpu.VMEM(packet, F32),
        pltpu.VMEM((PAIRS, 72, HD), F32),
        pltpu.VMEM((CHIPS, 72, HD), F32),
        pltpu.VMEM((CHIPS, 64, HD), F32),
        pltpu.VMEM((2, PAIRS, 64, HD), F32),
    ]
    whole = pl.BlockSpec(memory_space=pl.ANY)
    vmem = pl.BlockSpec(memory_space=pltpu.VMEM)
    wide = (TOK, PAIRS * HD)
    share = (TP, 32, HD)
    held = pl.pallas_call(
        main_kernel,
        out_shape=(
            pltpu.VMEM(wide, F32),
            pltpu.VMEM((TOK, HD), F32),
            pltpu.VMEM((TOK, HD), F32),
            pltpu.VMEM((2 * PAIRS, TOK), F32),
        ),
        in_specs=[whole] * 8,
        out_specs=(vmem,) * 4,
        scratch_shapes=[
            pltpu.VMEM(wide, BF16),
            pltpu.VMEM(wide, BF16),
            pltpu.VMEM((TOK, HD), BF16),
            pltpu.VMEM((TOK, HD), BF16),
            pltpu.VMEM((2 * PAIRS, TOK), F32),
            pltpu.VMEM((2 * PAIRS, TOK), F32),
            pltpu.VMEM((SEQ, TOK, HD), BF16),
            pltpu.VMEM((SEQ, TOK, HD), BF16),
            pltpu.VMEM((SEQ, 8 * TOK, TOK), F32),
            pltpu.VMEM((8 * TOK, HD), F32),
            pltpu.VMEM((2 * TOK, HD), F32),
            pltpu.VMEM((2 * TOK, HD), F32),
            pltpu.VMEM((8 * TOK, HD), BF16),
            pltpu.VMEM((16, TOK, TOK), F32),
            pltpu.VMEM((16, TOK, TOK), BF16),
            pltpu.VMEM((16, TOK, TOK), BF16),
            pltpu.VMEM(wide, F32),
            pltpu.VMEM(wide, F32),
            pltpu.VMEM(wide, F32),
            pltpu.VMEM((HD, TOK), BF16),
            pltpu.VMEM((HD, TOK), BF16),
            pltpu.VMEM((TOK, TOK), F32),
            pltpu.VMEM((TOK, HD), F32),
            pltpu.VMEM((PAIRS, 8, HD), F32),
            *exchange,
            pltpu.VMEM((PAIRS, HD, HD), F32),
            *exchange,
            pltpu.VMEM((TP, 64, HD), F32),
            pltpu.VMEM((TP, 64, HD), F32),
            pltpu.VMEM((64, HD), F32),
            pltpu.VMEM(share, F32),
            pltpu.VMEM(share, F32),
            pltpu.VMEM(share, F32),
            pltpu.VMEM((32, HD), F32),
            pltpu.VMEM(share, F32),
            dma((8,)),
            dma((16,)),
            dma((SEQ,)),
            dma((16,)),
            dma((SEQ,)),
            dma((8,)),
            dma((8,)),
            dma((2, CHIPS)),
            dma((2, CHIPS)),
            dma((2, CHIPS)),
            dma((2, CHIPS)),
            dma((4, TP)),
            dma((4, TP)),
        ],
        compiler_params=pltpu.CompilerParams(
            collective_id=0, has_side_effects=True, vmem_limit_bytes=61 * 1024 * 1024
        ),
        name="distill",
    )(query_rows, key_rows, value_rows, mixer_input, write_rows, read_rows, log_step, log_decay)
    return pl.pallas_call(
        write_kernel,
        out_shape=(
            jax.ShapeDtypeStruct(wide, F32),
            jax.ShapeDtypeStruct((TOK, HD), F32),
            jax.ShapeDtypeStruct((TOK, HD), F32),
            jax.ShapeDtypeStruct((2 * PAIRS, TOK), F32),
        ),
        in_specs=[vmem] * 4,
        out_specs=(whole,) * 4,
        scratch_shapes=[dma((4,))],
        compiler_params=pltpu.CompilerParams(vmem_limit_bytes=1024 * 1024),
        name="store",
    )(*held)


def solution(mesh):
    in_specs = (
        P("seq", "tp"),
        P("seq", "tp"),
        P("seq", "tp"),
        P("seq", "tp"),
        P("seq", None),
        P("seq", None),
        P("tp", "seq"),
        P("tp", "seq"),
    )
    out_specs = (P("seq", "tp"), P("seq", None), P("seq", None), P("tp", "seq"))
    return jax.shard_map(
        on_device, mesh=mesh, in_specs=in_specs, out_specs=out_specs, check_vma=False
    )
```

```python
import functools
import math

import jax
import jax.numpy as jnp
from jax import lax
from jax.experimental import pallas as pl
from jax.experimental.pallas import tpu as pltpu
from jax.sharding import PartitionSpec as P

MESH = pl.DeviceIdType.MESH
F32, BF16 = jnp.float32, jnp.bfloat16
TOK = 256
HD = 128
LOW = -1e30
SEQ = 16
CHIPS = 8
PAIRS = 8
TP = 8
SCALE = math.log2(math.e) / math.sqrt(HD)


def dot(a, b):
    return jnp.dot(a, b, preferred_element_type=F32)


def dot_nt(a, b):
    return lax.dot_general(a, b, (((1,), (1,)), ((), ())), preferred_element_type=F32)


def halves(a):
    high = a.astype(BF16)
    return high, (a - high.astype(F32)).astype(BF16)


def three(op, a, b):
    (ah, al), (bh, bl) = halves(a), halves(b)
    return op(ah, bh) + op(al, bh) + op(ah, bl)


def remote(src, dst, send_sem, recv_sem, axis, index):
    return pltpu.make_async_remote_copy(
        src_ref=src,
        dst_ref=dst,
        send_sem=send_sem,
        recv_sem=recv_sem,
        device_id={axis: index},
        device_id_type=MESH,
    )


def main_kernel(
    q_hbm,
    k_hbm,
    v_hbm,
    x_hbm,
    w_hbm,
    r_hbm,
    ls_hbm,
    ld_hbm,
    back,
    gw_ref,
    gr_ref,
    gls_ref,
    q_ref,
    x_ref,
    w_ref,
    r_ref,
    ls_ref,
    ld_ref,
    keys,
    values,
    scores,
    peak,
    total,
    mixed,
    taught,
    decay_buf,
    mix_high,
    mix_low,
    from_start,
    in_scale,
    local_y,
    wt_buf,
    rt_buf,
    pair_buf,
    sums,
    fwd_local,
    fwd_sibling,
    fwd_chip,
    fwd_got,
    fwd_out,
    fwd_in,
    state_in,
    bwd_local,
    bwd_sibling,
    bwd_chip,
    bwd_got,
    bwd_out,
    bwd_in,
    early,
    early_got,
    part,
    read_all,
    late,
    late_got,
    write_part,
    write_all,
    in_sem,
    key_send,
    key_recv,
    value_send,
    value_recv,
    sib_send,
    sib_recv,
    leg_send,
    leg_recv,
    ret_send,
    ret_recv,
    tp_send,
    tp_recv,
):
    me = lax.axis_index("seq")
    tp = lax.axis_index("tp")
    core = lax.rem(me, 2)
    chip = me // 2
    plane = lax.rem(chip, 2)
    row = me // 4
    sibling = me + 1 - 2 * core
    partner = me + 2 - 4 * plane
    above = lax.rem(me + 4, SEQ)
    below = lax.rem(me + 12, SEQ)
    far = lax.rem(me + 8, SEQ)
    above_p, below_p = lax.rem(partner + 4, SEQ), lax.rem(partner + 12, SEQ)
    far_p = lax.rem(partner + 8, SEQ)
    started = []

    barrier = pltpu.get_barrier_semaphore()
    for hop in range(1, SEQ):
        pl.semaphore_signal(
            barrier,
            inc=1,
            device_id={"seq": lax.rem(me + hop, SEQ)},
            device_id_type=MESH,
        )
    for hop in range(1, TP):
        pl.semaphore_signal(
            barrier,
            inc=1,
            device_id={"tp": lax.rem(tp + hop, TP)},
            device_id_type=MESH,
        )
    loads = [
        pltpu.make_async_copy(src, dst, in_sem.at[n])
        for n, (src, dst) in enumerate(
            (
                (k_hbm, keys.at[me]),
                (v_hbm, values.at[me]),
                (ld_hbm, ld_ref),
                (ls_hbm, ls_ref),
                (w_hbm, w_ref),
                (x_hbm, x_ref),
                (r_hbm, r_ref),
                (q_hbm, q_ref),
            )
        )
    ]
    for load in loads:
        load.start()

    def begin(copy):
        copy.start()
        started.append(copy)

    count = [0, 0]

    def pass_on(kind, index, *targets):
        store, send, recv = ((keys, key_send, key_recv), (values, value_send, value_recv))[kind]
        for target in targets:
            n = count[kind]
            count[kind] += 1
            begin(remote(store.at[index], store.at[index], send.at[n], recv.at[index], "seq", target))

    def arrived(kind, index):
        store, send, recv = ((keys, key_send, key_recv), (values, value_send, value_recv))[kind]
        remote(
            store.at[index], store.at[index], send.at[0], recv.at[index], "seq", sibling
        ).wait_recv()

    loads[0].wait()
    loads[1].wait()
    pl.semaphore_wait(barrier, SEQ + TP - 2)
    for kind in range(2):
        pass_on(kind, me, partner, above, below, sibling)

    def relay_one(kind):
        arrived(kind, partner)
        pass_on(kind, partner, above, below, sibling)
        arrived(kind, below)
        pass_on(kind, below, above, sibling)

    def relay_two(kind):
        arrived(kind, above_p)
        pass_on(kind, above_p, below, sibling)
        for index in (above, below_p):
            arrived(kind, index)
            pass_on(kind, index, sibling)

    def relay_three(kind):
        for index in (far, far_p):
            arrived(kind, index)
            pass_on(kind, index, sibling)

    rows = lax.broadcasted_iota(jnp.int32, (TOK, TOK), 0)
    cols = lax.broadcasted_iota(jnp.int32, (TOK, TOK), 1)
    causal = rows >= cols
    upper = jnp.where(rows <= cols, 1.0, 0.0).astype(BF16)
    for load in loads[2:6]:
        load.wait()
    log_decay = ld_ref[...]
    d1 = log_decay.astype(BF16)
    rest = log_decay - d1.astype(F32)
    d2 = rest.astype(BF16)
    d3 = (rest - d2.astype(F32)).astype(BF16)
    cum = dot(d1, upper) + dot(d2, upper) + dot(d3, upper)
    end = cum[:, TOK - 1 : TOK]
    row_term = ls_ref[...] - cum
    log_in = row_term + end
    columns = jnp.concatenate([cum, log_in, jnp.zeros((96, TOK), F32)], axis=0).T
    lane = lax.broadcasted_iota(jnp.int32, (TOK, HD), 1)
    first = lane < 64
    lane8 = lax.broadcasted_iota(jnp.int32, (8, HD), 1)

    def fwd_piece(g):
        two = pl.ds(2 * g, 2)
        return remote(
            fwd_local.at[two],
            fwd_sibling.at[two],
            sib_send.at[7 + g],
            sib_recv.at[7 + g],
            "seq",
            sibling,
        )

    wt_buf[...] = w_ref[...].T
    for t in range(PAIRS):
        a, b = 2 * t, 2 * t + 1
        at = slice(t * HD, (t + 1) * HD)
        scale = jnp.exp(
            jnp.where(first, columns[:, 16 + a : 17 + a], columns[:, 16 + b : 17 + b])
        )
        in_scale[:, at] = scale
        tile = jnp.where(lane8 < 64, end[a : a + 1, :], end[b : b + 1, :])
        high, low = halves(x_ref[:, at].astype(F32) * scale)
        state = dot(wt_buf[...], high) + dot(wt_buf[...], low)
        for half in range(2):
            fwd_local[t, half, 0:64] = state[half * 64 : (half + 1) * 64]
            fwd_local[t, half, 64:72] = tile
        if t % 2:
            begin(fwd_piece(t // 2))
    loads[6].wait()
    rt_buf[...] = r_ref[...].T
    inner = dot_nt(r_ref[...], w_ref[...])
    relay_one(0)

    def build(h):
        gap = columns[:, h : h + 1] + row_term[h : h + 1, :]
        decay = jnp.where(causal, jnp.exp(gap), 0.0)
        decay_buf[h] = decay
        high, low = halves(decay * inner)
        mix_high[h] = high
        mix_low[h] = low

    def chip_state(t, local, sib, out, early_first):
        mine, other = local[t, core], sib[t, core]
        early_core = jnp.where(core == 0, mine, other)
        late_core = jnp.where(core == 0, other, mine)
        if not early_first:
            span = jnp.where(core == 0, fwd_local[t, 0, 64:65], fwd_sibling[t, 0, 64:65])
            out[t] = late_core * jnp.exp(span) + early_core
            return
        out[t, 0:64] = early_core[0:64] * jnp.exp(late_core[64:65]) + late_core[0:64]
        out[t, 64:72] = early_core[64:72] + late_core[64:72]

    def leg(stage, t, chip_buf, got):
        return remote(
            chip_buf.at[t],
            got.at[chip],
            leg_send.at[stage, t],
            leg_recv.at[stage, chip],
            "seq",
            2 * t + core,
        )

    def send_leg(stage, t, chip_buf, got):
        @pl.when(chip != t)
        def _():
            leg(stage, t, chip_buf, got).start()

        @pl.when(chip == t)
        def _():
            got[t] = chip_buf[t]

    def scan_leg(stage, got, out, into, order):
        for hop in range(1, CHIPS):
            source = lax.rem(chip + hop, CHIPS)
            remote(
                got.at[source],
                got.at[source],
                leg_send.at[stage, 0],
                leg_recv.at[stage, source],
                "seq",
                sibling,
            ).wait_recv()
        running = jnp.zeros((64, HD), F32)
        for i in order:
            out[i] = running
            running = running * jnp.exp(fwd_got[i, 64:65]) + got[i, 0:64]
        into[core, chip] = out[chip]
        for hop in range(1, CHIPS):
            target = lax.rem(chip + hop, CHIPS)
            begin(
                remote(
                    out.at[target],
                    into.at[core, chip],
                    ret_send.at[stage, hop],
                    ret_recv.at[stage, chip],
                    "seq",
                    2 * target + core,
                )
            )

    def spread(stage, into):
        for hop in range(1, CHIPS):
            source = lax.rem(chip + hop, CHIPS)
            remote(
                into.at[core, source],
                into.at[core, source],
                ret_send.at[stage, 0],
                ret_recv.at[stage, source],
                "seq",
                sibling,
            ).wait_recv()
        begin(
            remote(
                into.at[core],
                into.at[core],
                sib_send.at[1 + stage],
                sib_recv.at[1 + stage],
                "seq",
                sibling,
            )
        )

    def spread_wait(stage, into):
        remote(
            into.at[1 - core],
            into.at[1 - core],
            sib_send.at[1 + stage],
            sib_recv.at[1 + stage],
            "seq",
            sibling,
        ).wait_recv()

    for g in range(4):
        fwd_piece(g).wait_recv()
        for t in (2 * g, 2 * g + 1):
            chip_state(t, fwd_local, fwd_sibling, fwd_chip, True)
            send_leg(0, t, fwd_chip, fwd_got)
    for t in range(PAIRS):
        a, b = 2 * t, 2 * t + 1
        from_start[:, t * HD : (t + 1) * HD] = jnp.exp(
            jnp.where(first, columns[:, a : a + 1], columns[:, b : b + 1])
        )
    for h in range(8):
        build(h)
    relay_one(1)
    relay_two(0)

    loads[7].wait()
    peak[...] = jnp.full(peak.shape, LOW, F32)

    def score_block(b, mask):
        kt = keys[b].T
        for h in range(8):
            at = slice(h * TOK, (h + 1) * TOK)
            s = dot(q_ref[:, h * HD : (h + 1) * HD], kt) * SCALE
            if mask:
                s = jnp.where(causal, s, LOW)
            scores[b, at] = s
            peak[at] = jnp.maximum(peak[at], jnp.maximum(s[:, :HD], s[:, HD:]))

    def score_other(shift):
        other = lax.rem(row + shift, 4)

        def step(i, carry):
            base = other * 4 + lax.rem(plane + i, 2) * 2
            arrived(0, base + 1 - core)

            @pl.when(other < row)
            def _():
                score_block(base, False)
                score_block(base + 1, False)

            return carry

        lax.fori_loop(0, 2, step, 0)

    def score_row(shift, low):
        def step(i, carry):
            flip = lax.rem(i, 2)
            b = (
                lax.rem(row + shift, 4) * 4
                + lax.rem(plane + i // 2, 2) * 2
                + lax.rem(core + flip, 2)
            )

            @pl.when(flip == 1)
            def _():
                arrived(0, b)

            @pl.when(b < me)
            def _():
                score_block(b, False)

            return carry

        lax.fori_loop(low, 4, step, 0)

    score_block(me, True)

    def blank(b, carry):
        scores[b] = jnp.full((8 * TOK, TOK), LOW, F32)
        return carry

    lax.fori_loop(me + 1, 4 * row + 4, blank, 0)

    for h in range(8, 16):
        build(h)
    score_row(0, 1)
    relay_two(1)
    relay_three(0)
    score_other(3)
    scan_leg(0, fwd_got, fwd_out, fwd_in, range(CHIPS))
    score_other(1)
    relay_three(1)

    def make_y(t, carry):
        at = pl.ds(pl.multiple_of(t * HD, HD), HD)
        x = x_ref[:, at]
        xa = jnp.where(first, x, jnp.zeros_like(x))
        xb = jnp.where(first, jnp.zeros_like(x), x)
        local_y[:, at] = (
            dot(mix_high[2 * t], xa)
            + dot(mix_low[2 * t], xa)
            + dot(mix_high[2 * t + 1], xb)
            + dot(mix_low[2 * t + 1], xb)
        )
        return carry

    lax.fori_loop(0, PAIRS, make_y, 0)
    score_other(2)
    for index in (me, partner, above, below, above_p, below_p, far, far_p):
        arrived(1, index + 1 - 2 * core)

    def weigh(g):
        at2 = slice(g * 2 * TOK, (g + 1) * 2 * TOK)
        top = jnp.max(peak[at2], axis=1, keepdims=True)
        total[...] = jnp.zeros(total.shape, F32)
        mixed[...] = jnp.zeros(mixed.shape, F32)

        def chunk(n, carry):
            low, folded = [], None
            for b in range(4):
                weights = jnp.exp2(scores[4 * n + b, at2] - top)
                low.append(weights.astype(BF16))
                both = weights[:, :HD] + weights[:, HD:]
                folded = both if folded is None else folded + both
            total[...] += folded
            shown = values[pl.ds(4 * n, 4)].reshape(4 * TOK, HD)
            mixed[...] += dot(jnp.concatenate(low, axis=1), shown)
            return carry

        lax.fori_loop(0, row + 1, chunk, 0)
        ratio = mixed[...] / jnp.sum(total[...], axis=1, keepdims=True)
        taught[at2] = ratio.astype(BF16)

    def meet(g):
        for t in (2 * g, 2 * g + 1):
            at = slice(t * HD, (t + 1) * HD)
            entering = jnp.concatenate([fwd_in[0, t], fwd_in[1, t]], axis=0)
            sib = fwd_sibling[t]
            sib_state = jnp.concatenate([sib[0, 0:64], sib[1, 0:64]], axis=0)
            entering = jnp.where(
                core == 1, entering * jnp.exp(sib[0, 64:65]) + sib_state, entering
            )
            state_in[t] = entering
            sh, sl = halves(entering)
            starts = from_start[:, at]
            carried = (dot(r_ref[...], sh) + dot(r_ref[...], sl)) * starts
            residual = local_y[:, at] + carried - taught[t * TOK : (t + 1) * TOK].astype(F32)
            local_y[:, at] = residual
            wh, wl = halves(residual * starts)
            adjoint = dot(rt_buf[...], wh) + dot(rt_buf[...], wl)
            for half in range(2):
                bwd_local[t, half] = adjoint[half * 64 : (half + 1) * 64]
        two = pl.ds(2 * g, 2)
        begin(
            remote(
                bwd_local.at[two],
                bwd_sibling.at[two],
                sib_send.at[3 + g],
                sib_recv.at[3 + g],
                "seq",
                sibling,
            )
        )

    def hand_over(g):
        two = pl.ds(2 * g, 2)
        remote(
            bwd_sibling.at[two],
            bwd_sibling.at[two],
            sib_send.at[3 + g],
            sib_recv.at[3 + g],
            "seq",
            sibling,
        ).wait_recv()
        for t in (2 * g, 2 * g + 1):
            chip_state(t, bwd_local, bwd_sibling, bwd_chip, False)
            send_leg(1, t, bwd_chip, bwd_got)

    def local_terms(t, carry):
        at = pl.ds(pl.multiple_of(t * HD, HD), HD)
        residual = local_y[:, at]
        xt = x_ref[:, at].T
        for side, own in ((0, first), (1, ~first)):
            rh, rl = halves(jnp.where(own, residual, 0.0))
            pair_buf[...] += decay_buf[2 * t + side] * (dot(rh, xt) + dot(rl, xt))
        return carry

    def back_terms(t, carry):
        at = pl.ds(pl.multiple_of(t * HD, HD), HD)
        residual_t = local_y[:, at].T
        rh, rl = halves(residual_t)
        pieces = []
        for side in range(2):
            own = slice(side * 64, (side + 1) * 64)
            both = jnp.concatenate([rh[own], rl[own]], axis=0)
            product = dot(both, mix_high[2 * t + side])
            pieces.append(product[0:64] + product[64:128] + dot(rh[own], mix_low[2 * t + side]))
        back[:, at] = jnp.concatenate(pieces, axis=0).T
        return carry

    def read_terms(t, carry):
        at = pl.ds(pl.multiple_of(t * HD, HD), HD)
        weighted = local_y[:, at] * from_start[:, at]
        sums[...] += three(dot_nt, weighted, state_in[t])
        return carry

    pair_buf[...] = jnp.zeros(pair_buf.shape, F32)
    sums[...] = jnp.zeros(sums.shape, F32)
    weigh(0)
    weigh(1)
    spread(0, fwd_in)
    weigh(2)
    spread_wait(0, fwd_in)
    meet(0)
    meet(1)
    hand_over(0)
    meet(2)
    hand_over(1)
    weigh(3)
    hand_over(2)
    meet(3)
    lax.fori_loop(0, 4, local_terms, 0)
    hand_over(3)
    lax.fori_loop(4, PAIRS, local_terms, 0)
    lax.fori_loop(0, PAIRS, read_terms, 0)
    ph, pw = halves(pair_buf[...])
    grad_read = sums[...] + dot(ph, w_ref[...]) + dot(pw, w_ref[...])
    th, tl = halves(pair_buf[...].T)
    sums[...] = dot(th, r_ref[...]) + dot(tl, r_ref[...])
    for i in range(TP):
        early[i] = grad_read[i * 32 : (i + 1) * 32]

    def scatter(stage, source, got):
        got[tp] = source[tp]
        for hop in range(1, TP):
            to = lax.rem(tp + hop, TP)
            begin(
                remote(
                    source.at[to], got.at[tp], tp_send.at[stage, hop], tp_recv.at[stage, tp], "tp", to
                )
            )

    def gather(stage, source, got):
        got[tp] = source[...]
        for hop in range(1, TP):
            to = lax.rem(tp + hop, TP)
            begin(
                remote(source, got.at[tp], tp_send.at[stage, hop], tp_recv.at[stage, tp], "tp", to)
            )

    def collect(stage, got):
        for hop in range(1, TP):
            source = lax.rem(tp + hop, TP)
            remote(
                got.at[source],
                got.at[source],
                tp_send.at[stage, 0],
                tp_recv.at[stage, source],
                "tp",
                source,
            ).wait_recv()

    scatter(0, early, early_got)
    scan_leg(1, bwd_got, bwd_out, bwd_in, range(CHIPS - 1, -1, -1))
    lax.fori_loop(0, PAIRS, back_terms, 0)
    collect(0, early_got)
    acc = early_got[0]
    for i in range(1, TP):
        acc = acc + early_got[i]
    part[...] = acc
    gather(1, part, read_all)

    def across(t, half):
        return remote(
            bwd_in.at[half, t],
            bwd_in.at[half, t],
            sib_send.at[11 + t],
            sib_recv.at[11 + t],
            "seq",
            sibling,
        )

    begin(across(chip, core))
    for hop in range(1, CHIPS):
        source = lax.rem(chip + hop, CHIPS)
        remote(
            bwd_in.at[core, source],
            bwd_in.at[core, source],
            ret_send.at[1, 0],
            ret_recv.at[1, source],
            "seq",
            sibling,
        ).wait_recv()
        begin(across(source, core))

    def carry_terms(i, carry):
        t = lax.rem(chip + i, CHIPS)
        across(t, 1 - core).wait_recv()
        at = pl.ds(pl.multiple_of(t * HD, HD), HD)
        arriving = jnp.concatenate([bwd_in[0, t], bwd_in[1, t]], axis=0)
        sib_state = jnp.concatenate([bwd_sibling[t, 0], bwd_sibling[t, 1]], axis=0)
        arriving = jnp.where(
            core == 0, arriving * jnp.exp(fwd_sibling[t, 0, 64:65]) + sib_state, arriving
        )
        state_in[t] = arriving
        sums[...] += three(dot_nt, x_ref[:, at].astype(F32) * in_scale[:, at], arriving)
        return carry

    lax.fori_loop(0, PAIRS, carry_terms, 0)
    for i in range(TP):
        late[i] = sums[i * 32 : (i + 1) * 32]
    scatter(2, late, late_got)

    row16 = lax.broadcasted_iota(jnp.int32, (16, HD), 0)
    lane16 = lax.broadcasted_iota(jnp.int32, (16, HD), 1)
    gls_ref[...] = jnp.zeros(gls_ref.shape, F32)

    def finish(t, carry):
        at = pl.ds(pl.multiple_of(t * HD, HD), HD)
        ah, al = halves(state_in[t])
        grad = back[:, at] + in_scale[:, at] * (dot(w_ref[...], ah) + dot(w_ref[...], al))
        back[:, at] = grad
        gh, gl = halves(x_ref[:, at].astype(F32) * grad)
        pick = jnp.where(row16 == 2 * t + lane16 // 64, 1.0, 0.0).astype(BF16)
        gls_ref[...] += dot_nt(pick, gh) + dot_nt(pick, gl)
        return carry

    lax.fori_loop(0, PAIRS, finish, 0)
    collect(1, read_all)
    for i in range(TP):
        gr_ref[i * 32 : (i + 1) * 32] = read_all[i]
    collect(2, late_got)
    acc = late_got[0]
    for i in range(1, TP):
        acc = acc + late_got[i]
    write_part[...] = acc
    gather(3, write_part, write_all)
    for copy in started:
        copy.wait_send()
    for t in range(PAIRS):

        @pl.when(chip != t)
        def _():
            leg(0, t, fwd_chip, fwd_got).wait_send()
            leg(1, t, bwd_chip, bwd_got).wait_send()

    collect(3, write_all)
    for i in range(TP):
        gw_ref[i * 32 : (i + 1) * 32] = write_all[i]


def write_kernel(*refs):
    copies = [
        pltpu.make_async_copy(src, dst, refs[8].at[n])
        for n, (src, dst) in enumerate(zip(refs[0:4], refs[4:8]))
    ]
    for copy in copies:
        copy.start()
    for copy in copies:
        copy.wait()


def on_device(
    query_rows, key_rows, value_rows, mixer_input, write_rows, read_rows, log_step, log_decay
):
    dma = pltpu.SemaphoreType.DMA
    packet = (PAIRS, 2, 72, HD)
    exchange = [
        pltpu.VMEM(packet, F32),
        pltpu.VMEM(packet, F32),
        pltpu.VMEM((PAIRS, 72, HD), F32),
        pltpu.VMEM((CHIPS, 72, HD), F32),
        pltpu.VMEM((CHIPS, 64, HD), F32),
        pltpu.VMEM((2, PAIRS, 64, HD), F32),
    ]
    whole = pl.BlockSpec(memory_space=pl.ANY)
    vmem = pl.BlockSpec(memory_space=pltpu.VMEM)
    wide = (TOK, PAIRS * HD)
    share = (TP, 32, HD)
    held = pl.pallas_call(
        main_kernel,
        out_shape=(
            pltpu.VMEM(wide, F32),
            pltpu.VMEM((TOK, HD), F32),
            pltpu.VMEM((TOK, HD), F32),
            pltpu.VMEM((2 * PAIRS, TOK), F32),
        ),
        in_specs=[whole] * 8,
        out_specs=(vmem,) * 4,
        scratch_shapes=[
            pltpu.VMEM(wide, BF16),
            pltpu.VMEM(wide, BF16),
            pltpu.VMEM((TOK, HD), BF16),
            pltpu.VMEM((TOK, HD), BF16),
            pltpu.VMEM((2 * PAIRS, TOK), F32),
            pltpu.VMEM((2 * PAIRS, TOK), F32),
            pltpu.VMEM((SEQ, TOK, HD), BF16),
            pltpu.VMEM((SEQ, TOK, HD), BF16),
            pltpu.VMEM((SEQ, 8 * TOK, TOK), F32),
            pltpu.VMEM((8 * TOK, HD), F32),
            pltpu.VMEM((2 * TOK, HD), F32),
            pltpu.VMEM((2 * TOK, HD), F32),
            pltpu.VMEM((8 * TOK, HD), BF16),
            pltpu.VMEM((16, TOK, TOK), F32),
            pltpu.VMEM((16, TOK, TOK), BF16),
            pltpu.VMEM((16, TOK, TOK), BF16),
            pltpu.VMEM(wide, F32),
            pltpu.VMEM(wide, F32),
            pltpu.VMEM(wide, F32),
            pltpu.VMEM((HD, TOK), BF16),
            pltpu.VMEM((HD, TOK), BF16),
            pltpu.VMEM((TOK, TOK), F32),
            pltpu.VMEM((TOK, HD), F32),
            *exchange,
            pltpu.VMEM((PAIRS, HD, HD), F32),
            pltpu.VMEM((PAIRS, 2, 64, HD), F32),
            pltpu.VMEM((PAIRS, 2, 64, HD), F32),
            pltpu.VMEM((PAIRS, 64, HD), F32),
            pltpu.VMEM((CHIPS, 64, HD), F32),
            pltpu.VMEM((CHIPS, 64, HD), F32),
            pltpu.VMEM((2, PAIRS, 64, HD), F32),
            pltpu.VMEM(share, F32),
            pltpu.VMEM(share, F32),
            pltpu.VMEM((32, HD), F32),
            pltpu.VMEM(share, F32),
            pltpu.VMEM(share, F32),
            pltpu.VMEM(share, F32),
            pltpu.VMEM((32, HD), F32),
            pltpu.VMEM(share, F32),
            dma((8,)),
            dma((16,)),
            dma((SEQ,)),
            dma((16,)),
            dma((SEQ,)),
            dma((19,)),
            dma((19,)),
            dma((2, CHIPS)),
            dma((2, CHIPS)),
            dma((2, CHIPS)),
            dma((2, CHIPS)),
            dma((4, TP)),
            dma((4, TP)),
        ],
        compiler_params=pltpu.CompilerParams(
            collective_id=0, has_side_effects=True, vmem_limit_bytes=61 * 1024 * 1024
        ),
        name="distill",
    )(query_rows, key_rows, value_rows, mixer_input, write_rows, read_rows, log_step, log_decay)
    return pl.pallas_call(
        write_kernel,
        out_shape=(
            jax.ShapeDtypeStruct(wide, F32),
            jax.ShapeDtypeStruct((TOK, HD), F32),
            jax.ShapeDtypeStruct((TOK, HD), F32),
            jax.ShapeDtypeStruct((2 * PAIRS, TOK), F32),
        ),
        in_specs=[vmem] * 4,
        out_specs=(whole,) * 4,
        scratch_shapes=[dma((4,))],
        compiler_params=pltpu.CompilerParams(vmem_limit_bytes=1024 * 1024),
        name="store",
    )(*held)


def solution(mesh):
    in_specs = (
        P("seq", "tp"),
        P("seq", "tp"),
        P("seq", "tp"),
        P("seq", "tp"),
        P("seq", None),
        P("seq", None),
        P("tp", "seq"),
        P("tp", "seq"),
    )
    out_specs = (P("seq", "tp"), P("seq", None), P("seq", None), P("tp", "seq"))
    return jax.shard_map(
        on_device, mesh=mesh, in_specs=in_specs, out_specs=out_specs, check_vma=False
    )
```

```python
import functools
import math

import jax
import jax.numpy as jnp
from jax import lax
from jax.experimental import pallas as pl
from jax.experimental.pallas import tpu as pltpu
from jax.sharding import PartitionSpec as P

MESH = pl.DeviceIdType.MESH
F32, BF16 = jnp.float32, jnp.bfloat16
TOK = 256
HD = 128
LOW = -1e30
SEQ = 16
CHIPS = 8
PAIRS = 8
TP = 8
SCALE = math.log2(math.e) / math.sqrt(HD)


def dot(a, b):
    return jnp.dot(a, b, preferred_element_type=F32)


def dot_nt(a, b):
    return lax.dot_general(a, b, (((1,), (1,)), ((), ())), preferred_element_type=F32)


def halves(a):
    high = a.astype(BF16)
    return high, (a - high.astype(F32)).astype(BF16)


def three(op, a, b):
    (ah, al), (bh, bl) = halves(a), halves(b)
    return op(ah, bh) + op(al, bh) + op(ah, bl)


def remote(src, dst, send_sem, recv_sem, axis, index):
    return pltpu.make_async_remote_copy(
        src_ref=src,
        dst_ref=dst,
        send_sem=send_sem,
        recv_sem=recv_sem,
        device_id={axis: index},
        device_id_type=MESH,
    )


def main_kernel(
    q_hbm,
    k_hbm,
    v_hbm,
    x_hbm,
    w_hbm,
    r_hbm,
    ls_hbm,
    ld_hbm,
    back,
    gw_ref,
    gr_ref,
    gls_ref,
    q_ref,
    x_ref,
    w_ref,
    r_ref,
    ls_ref,
    ld_ref,
    keys,
    values,
    scores,
    peak,
    total,
    mixed,
    taught,
    decay_buf,
    mix_high,
    mix_low,
    from_start,
    in_scale,
    local_y,
    wt_buf,
    rt_buf,
    pair_buf,
    sums,
    fwd_local,
    fwd_sibling,
    fwd_chip,
    fwd_got,
    fwd_out,
    fwd_in,
    state_in,
    bwd_local,
    bwd_sibling,
    bwd_chip,
    bwd_got,
    bwd_out,
    bwd_in,
    early,
    early_got,
    part,
    read_all,
    late,
    late_got,
    write_part,
    write_all,
    in_sem,
    key_send,
    key_recv,
    value_send,
    value_recv,
    sib_send,
    sib_recv,
    leg_send,
    leg_recv,
    ret_send,
    ret_recv,
    tp_send,
    tp_recv,
):
    me = lax.axis_index("seq")
    tp = lax.axis_index("tp")
    core = lax.rem(me, 2)
    chip = me // 2
    plane = lax.rem(chip, 2)
    row = me // 4
    sibling = me + 1 - 2 * core
    partner = me + 2 - 4 * plane
    above = lax.rem(me + 4, SEQ)
    below = lax.rem(me + 12, SEQ)
    far = lax.rem(me + 8, SEQ)
    above_p, below_p = lax.rem(partner + 4, SEQ), lax.rem(partner + 12, SEQ)
    far_p = lax.rem(partner + 8, SEQ)
    started = []

    barrier = pltpu.get_barrier_semaphore()
    for hop in range(1, SEQ):
        pl.semaphore_signal(
            barrier,
            inc=1,
            device_id={"seq": lax.rem(me + hop, SEQ)},
            device_id_type=MESH,
        )
    for hop in range(1, TP):
        pl.semaphore_signal(
            barrier,
            inc=1,
            device_id={"tp": lax.rem(tp + hop, TP)},
            device_id_type=MESH,
        )
    loads = [
        pltpu.make_async_copy(src, dst, in_sem.at[n])
        for n, (src, dst) in enumerate(
            (
                (k_hbm, keys.at[me]),
                (v_hbm, values.at[me]),
                (ld_hbm, ld_ref),
                (ls_hbm, ls_ref),
                (w_hbm, w_ref),
                (x_hbm, x_ref),
                (r_hbm, r_ref),
                (q_hbm, q_ref),
            )
        )
    ]
    for load in loads:
        load.start()

    def begin(copy):
        copy.start()
        started.append(copy)

    count = [0, 0]

    def pass_on(kind, index, *targets):
        store, send, recv = ((keys, key_send, key_recv), (values, value_send, value_recv))[kind]
        for target in targets:
            n = count[kind]
            count[kind] += 1
            begin(remote(store.at[index], store.at[index], send.at[n], recv.at[index], "seq", target))

    def arrived(kind, index):
        store, send, recv = ((keys, key_send, key_recv), (values, value_send, value_recv))[kind]
        remote(
            store.at[index], store.at[index], send.at[0], recv.at[index], "seq", sibling
        ).wait_recv()

    loads[0].wait()
    loads[1].wait()
    pl.semaphore_wait(barrier, SEQ + TP - 2)
    for kind in range(2):
        pass_on(kind, me, partner, above, below, sibling)

    def relay_one(kind):
        arrived(kind, partner)
        pass_on(kind, partner, above, below, sibling)
        arrived(kind, below)
        pass_on(kind, below, above, sibling)

    def relay_two(kind):
        arrived(kind, above_p)
        pass_on(kind, above_p, below, sibling)
        for index in (above, below_p):
            arrived(kind, index)
            pass_on(kind, index, sibling)

    def relay_three(kind):
        for index in (far, far_p):
            arrived(kind, index)
            pass_on(kind, index, sibling)

    rows = lax.broadcasted_iota(jnp.int32, (TOK, TOK), 0)
    cols = lax.broadcasted_iota(jnp.int32, (TOK, TOK), 1)
    causal = rows >= cols
    upper = jnp.where(rows <= cols, 1.0, 0.0).astype(BF16)
    for load in loads[2:6]:
        load.wait()
    log_decay = ld_ref[...]
    d1 = log_decay.astype(BF16)
    rest = log_decay - d1.astype(F32)
    d2 = rest.astype(BF16)
    d3 = (rest - d2.astype(F32)).astype(BF16)
    cum = dot(d1, upper) + dot(d2, upper) + dot(d3, upper)
    end = cum[:, TOK - 1 : TOK]
    row_term = ls_ref[...] - cum
    log_in = row_term + end
    columns = jnp.concatenate([cum, log_in, jnp.zeros((96, TOK), F32)], axis=0).T
    lane = lax.broadcasted_iota(jnp.int32, (TOK, HD), 1)
    first = lane < 64
    lane8 = lax.broadcasted_iota(jnp.int32, (8, HD), 1)

    def fwd_piece(g):
        two = pl.ds(2 * g, 2)
        return remote(
            fwd_local.at[two],
            fwd_sibling.at[two],
            sib_send.at[7 + g],
            sib_recv.at[7 + g],
            "seq",
            sibling,
        )

    wt_buf[...] = w_ref[...].T
    for t in range(PAIRS):
        a, b = 2 * t, 2 * t + 1
        at = slice(t * HD, (t + 1) * HD)
        scale = jnp.exp(
            jnp.where(first, columns[:, 16 + a : 17 + a], columns[:, 16 + b : 17 + b])
        )
        in_scale[:, at] = scale
        tile = jnp.where(lane8 < 64, end[a : a + 1, :], end[b : b + 1, :])
        high, low = halves(x_ref[:, at].astype(F32) * scale)
        state = dot(wt_buf[...], high) + dot(wt_buf[...], low)
        for half in range(2):
            fwd_local[t, half, 0:64] = state[half * 64 : (half + 1) * 64]
            fwd_local[t, half, 64:72] = tile
        if t % 2:
            begin(fwd_piece(t // 2))
    loads[6].wait()
    rt_buf[...] = r_ref[...].T
    inner = dot_nt(r_ref[...], w_ref[...])
    relay_one(0)

    def build(h):
        gap = columns[:, h : h + 1] + row_term[h : h + 1, :]
        decay = jnp.where(causal, jnp.exp(gap), 0.0)
        decay_buf[h] = decay
        high, low = halves(decay * inner)
        mix_high[h] = high
        mix_low[h] = low

    def chip_state(t, local, sib, out, early_first):
        mine, other = local[t, core], sib[t, core]
        early_core = jnp.where(core == 0, mine, other)
        late_core = jnp.where(core == 0, other, mine)
        if not early_first:
            span = jnp.where(core == 0, fwd_local[t, 0, 64:65], fwd_sibling[t, 0, 64:65])
            out[t] = late_core * jnp.exp(span) + early_core
            return
        out[t, 0:64] = early_core[0:64] * jnp.exp(late_core[64:65]) + late_core[0:64]
        out[t, 64:72] = early_core[64:72] + late_core[64:72]

    def leg(stage, t, chip_buf, got):
        return remote(
            chip_buf.at[t],
            got.at[chip],
            leg_send.at[stage, t],
            leg_recv.at[stage, chip],
            "seq",
            2 * t + core,
        )

    def send_leg(stage, t, chip_buf, got):
        @pl.when(chip != t)
        def _():
            leg(stage, t, chip_buf, got).start()

        @pl.when(chip == t)
        def _():
            got[t] = chip_buf[t]

    def scan_leg(stage, got, out, into, order):
        for hop in range(1, CHIPS):
            source = lax.rem(chip + hop, CHIPS)
            remote(
                got.at[source],
                got.at[source],
                leg_send.at[stage, 0],
                leg_recv.at[stage, source],
                "seq",
                sibling,
            ).wait_recv()
        running = jnp.zeros((64, HD), F32)
        for i in order:
            out[i] = running
            running = running * jnp.exp(fwd_got[i, 64:65]) + got[i, 0:64]
        into[core, chip] = out[chip]
        for hop in range(1, CHIPS):
            target = lax.rem(chip + hop, CHIPS)
            begin(
                remote(
                    out.at[target],
                    into.at[core, chip],
                    ret_send.at[stage, hop],
                    ret_recv.at[stage, chip],
                    "seq",
                    2 * target + core,
                )
            )

    def spread(stage, into):
        for hop in range(1, CHIPS):
            source = lax.rem(chip + hop, CHIPS)
            remote(
                into.at[core, source],
                into.at[core, source],
                ret_send.at[stage, 0],
                ret_recv.at[stage, source],
                "seq",
                sibling,
            ).wait_recv()
        begin(
            remote(
                into.at[core],
                into.at[core],
                sib_send.at[1 + stage],
                sib_recv.at[1 + stage],
                "seq",
                sibling,
            )
        )

    def spread_wait(stage, into):
        remote(
            into.at[1 - core],
            into.at[1 - core],
            sib_send.at[1 + stage],
            sib_recv.at[1 + stage],
            "seq",
            sibling,
        ).wait_recv()

    for g in range(4):
        fwd_piece(g).wait_recv()
        for t in (2 * g, 2 * g + 1):
            chip_state(t, fwd_local, fwd_sibling, fwd_chip, True)
            send_leg(0, t, fwd_chip, fwd_got)
    for t in range(PAIRS):
        a, b = 2 * t, 2 * t + 1
        from_start[:, t * HD : (t + 1) * HD] = jnp.exp(
            jnp.where(first, columns[:, a : a + 1], columns[:, b : b + 1])
        )
    for h in range(8):
        build(h)
    relay_one(1)
    relay_two(0)

    loads[7].wait()
    peak[...] = jnp.full(peak.shape, LOW, F32)

    def score_block(b, mask):
        kt = keys[b].T
        for h in range(8):
            at = slice(h * TOK, (h + 1) * TOK)
            s = dot(q_ref[:, h * HD : (h + 1) * HD], kt) * SCALE
            if mask:
                s = jnp.where(causal, s, LOW)
            scores[b, at] = s
            peak[at] = jnp.maximum(peak[at], jnp.maximum(s[:, :HD], s[:, HD:]))

    def score_other(shift):
        other = lax.rem(row + shift, 4)

        def step(i, carry):
            base = other * 4 + lax.rem(plane + i, 2) * 2
            arrived(0, base + 1 - core)

            @pl.when(other < row)
            def _():
                score_block(base, False)
                score_block(base + 1, False)

            return carry

        lax.fori_loop(0, 2, step, 0)

    def score_row(shift, low):
        def step(i, carry):
            flip = lax.rem(i, 2)
            b = (
                lax.rem(row + shift, 4) * 4
                + lax.rem(plane + i // 2, 2) * 2
                + lax.rem(core + flip, 2)
            )

            @pl.when(flip == 1)
            def _():
                arrived(0, b)

            @pl.when(b < me)
            def _():
                score_block(b, False)

            return carry

        lax.fori_loop(low, 4, step, 0)

    score_block(me, True)

    def blank(b, carry):
        scores[b] = jnp.full((8 * TOK, TOK), LOW, F32)
        return carry

    lax.fori_loop(me + 1, 4 * row + 4, blank, 0)

    for h in range(8, 16):
        build(h)
    score_row(0, 1)
    relay_two(1)
    relay_three(0)
    score_other(3)
    scan_leg(0, fwd_got, fwd_out, fwd_in, range(CHIPS))
    score_other(1)
    relay_three(1)

    def make_y(t, carry):
        at = pl.ds(pl.multiple_of(t * HD, HD), HD)
        x = x_ref[:, at]
        xa = jnp.where(first, x, jnp.zeros_like(x))
        xb = jnp.where(first, jnp.zeros_like(x), x)
        local_y[:, at] = (
            dot(mix_high[2 * t], xa)
            + dot(mix_low[2 * t], xa)
            + dot(mix_high[2 * t + 1], xb)
            + dot(mix_low[2 * t + 1], xb)
        )
        return carry

    lax.fori_loop(0, PAIRS, make_y, 0)
    score_other(2)
    for index in (me, partner, above, below, above_p, below_p, far, far_p):
        arrived(1, index + 1 - 2 * core)

    def weigh(g):
        at2 = slice(g * 2 * TOK, (g + 1) * 2 * TOK)
        top = jnp.max(peak[at2], axis=1, keepdims=True)
        total[...] = jnp.zeros(total.shape, F32)
        mixed[...] = jnp.zeros(mixed.shape, F32)

        def chunk(n, carry):
            low, folded = [], None
            for b in range(4):
                weights = jnp.exp2(scores[4 * n + b, at2] - top)
                low.append(weights.astype(BF16))
                both = weights[:, :HD] + weights[:, HD:]
                folded = both if folded is None else folded + both
            total[...] += folded
            shown = values[pl.ds(4 * n, 4)].reshape(4 * TOK, HD)
            mixed[...] += dot(jnp.concatenate(low, axis=1), shown)
            return carry

        lax.fori_loop(0, row + 1, chunk, 0)
        ratio = mixed[...] / jnp.sum(total[...], axis=1, keepdims=True)
        taught[at2] = ratio.astype(BF16)

    def meet(g):
        for t in (2 * g, 2 * g + 1):
            at = slice(t * HD, (t + 1) * HD)
            entering = jnp.concatenate([fwd_in[0, t], fwd_in[1, t]], axis=0)
            sib = fwd_sibling[t]
            sib_state = jnp.concatenate([sib[0, 0:64], sib[1, 0:64]], axis=0)
            entering = jnp.where(
                core == 1, entering * jnp.exp(sib[0, 64:65]) + sib_state, entering
            )
            state_in[t] = entering
            sh, sl = halves(entering)
            starts = from_start[:, at]
            carried = (dot(r_ref[...], sh) + dot(r_ref[...], sl)) * starts
            residual = local_y[:, at] + carried - taught[t * TOK : (t + 1) * TOK].astype(F32)
            local_y[:, at] = residual
            wh, wl = halves(residual * starts)
            adjoint = dot(rt_buf[...], wh) + dot(rt_buf[...], wl)
            for half in range(2):
                bwd_local[t, half] = adjoint[half * 64 : (half + 1) * 64]
        two = pl.ds(2 * g, 2)
        begin(
            remote(
                bwd_local.at[two],
                bwd_sibling.at[two],
                sib_send.at[3 + g],
                sib_recv.at[3 + g],
                "seq",
                sibling,
            )
        )

    def hand_over(g):
        two = pl.ds(2 * g, 2)
        remote(
            bwd_sibling.at[two],
            bwd_sibling.at[two],
            sib_send.at[3 + g],
            sib_recv.at[3 + g],
            "seq",
            sibling,
        ).wait_recv()
        for t in (2 * g, 2 * g + 1):
            chip_state(t, bwd_local, bwd_sibling, bwd_chip, False)
            send_leg(1, t, bwd_chip, bwd_got)

    def local_terms(t, carry):
        at = pl.ds(pl.multiple_of(t * HD, HD), HD)
        residual = local_y[:, at]
        xt = x_ref[:, at].T
        for side, own in ((0, first), (1, ~first)):
            rh, rl = halves(jnp.where(own, residual, 0.0))
            pair_buf[...] += decay_buf[2 * t + side] * (dot(rh, xt) + dot(rl, xt))
        return carry

    def back_terms(t, carry):
        at = pl.ds(pl.multiple_of(t * HD, HD), HD)
        residual_t = local_y[:, at].T
        rh, rl = halves(residual_t)
        pieces = []
        for side in range(2):
            own = slice(side * 64, (side + 1) * 64)
            both = jnp.concatenate([rh[own], rl[own]], axis=0)
            product = dot(both, mix_high[2 * t + side])
            pieces.append(product[0:64] + product[64:128] + dot(rh[own], mix_low[2 * t + side]))
        back[:, at] = jnp.concatenate(pieces, axis=0).T
        high, low = halves(x_ref[:, at].astype(F32) * in_scale[:, at])
        q_ref[:, at] = high
        taught[pl.ds(pl.multiple_of(t * TOK, TOK), TOK)] = low
        return carry

    def read_terms(t, carry):
        at = pl.ds(pl.multiple_of(t * HD, HD), HD)
        weighted = local_y[:, at] * from_start[:, at]
        sums[...] += three(dot_nt, weighted, state_in[t])
        return carry

    pair_buf[...] = jnp.zeros(pair_buf.shape, F32)
    sums[...] = jnp.zeros(sums.shape, F32)
    weigh(0)
    weigh(1)
    spread(0, fwd_in)
    weigh(2)
    spread_wait(0, fwd_in)
    meet(0)
    meet(1)
    hand_over(0)
    meet(2)
    hand_over(1)
    weigh(3)
    hand_over(2)
    meet(3)
    lax.fori_loop(0, 4, local_terms, 0)
    hand_over(3)
    lax.fori_loop(4, PAIRS, local_terms, 0)
    lax.fori_loop(0, PAIRS, read_terms, 0)
    ph, pw = halves(pair_buf[...])
    grad_read = sums[...] + dot(ph, w_ref[...]) + dot(pw, w_ref[...])
    th, tl = halves(pair_buf[...].T)
    sums[...] = dot(th, r_ref[...]) + dot(tl, r_ref[...])
    for i in range(TP):
        early[i] = grad_read[i * 32 : (i + 1) * 32]

    def scatter(stage, source, got):
        got[tp] = source[tp]
        for hop in range(1, TP):
            to = lax.rem(tp + hop, TP)
            begin(
                remote(
                    source.at[to], got.at[tp], tp_send.at[stage, hop], tp_recv.at[stage, tp], "tp", to
                )
            )

    def gather(stage, source, got):
        got[tp] = source[...]
        for hop in range(1, TP):
            to = lax.rem(tp + hop, TP)
            begin(
                remote(source, got.at[tp], tp_send.at[stage, hop], tp_recv.at[stage, tp], "tp", to)
            )

    def collect(stage, got):
        for hop in range(1, TP):
            source = lax.rem(tp + hop, TP)
            remote(
                got.at[source],
                got.at[source],
                tp_send.at[stage, 0],
                tp_recv.at[stage, source],
                "tp",
                source,
            ).wait_recv()

    scatter(0, early, early_got)
    scan_leg(1, bwd_got, bwd_out, bwd_in, range(CHIPS - 1, -1, -1))
    lax.fori_loop(0, PAIRS, back_terms, 0)
    collect(0, early_got)
    acc = early_got[0]
    for i in range(1, TP):
        acc = acc + early_got[i]
    part[...] = acc
    gather(1, part, read_all)

    def across(t, half):
        return remote(
            bwd_in.at[half, t],
            bwd_in.at[half, t],
            sib_send.at[11 + t],
            sib_recv.at[11 + t],
            "seq",
            sibling,
        )

    begin(across(chip, core))
    for hop in range(1, CHIPS):
        source = lax.rem(chip + hop, CHIPS)
        remote(
            bwd_in.at[core, source],
            bwd_in.at[core, source],
            ret_send.at[1, 0],
            ret_recv.at[1, source],
            "seq",
            sibling,
        ).wait_recv()
        begin(across(source, core))

    def carry_terms(i, carry):
        t = lax.rem(chip + i, CHIPS)
        across(t, 1 - core).wait_recv()
        at = pl.ds(pl.multiple_of(t * HD, HD), HD)
        arriving = jnp.concatenate([bwd_in[0, t], bwd_in[1, t]], axis=0)
        sib_state = jnp.concatenate([bwd_sibling[t, 0], bwd_sibling[t, 1]], axis=0)
        arriving = jnp.where(
            core == 0, arriving * jnp.exp(fwd_sibling[t, 0, 64:65]) + sib_state, arriving
        )
        state_in[t] = arriving
        ah, al = halves(arriving)
        high, low = q_ref[:, at], taught[pl.ds(pl.multiple_of(t * TOK, TOK), TOK)]
        sums[...] += dot_nt(high, ah) + dot_nt(low, ah) + dot_nt(high, al)
        return carry

    lax.fori_loop(0, PAIRS, carry_terms, 0)
    for i in range(TP):
        late[i] = sums[i * 32 : (i + 1) * 32]
    scatter(2, late, late_got)

    row16 = lax.broadcasted_iota(jnp.int32, (16, HD), 0)
    lane16 = lax.broadcasted_iota(jnp.int32, (16, HD), 1)
    gls_ref[...] = jnp.zeros(gls_ref.shape, F32)

    def finish(t, carry):
        at = pl.ds(pl.multiple_of(t * HD, HD), HD)
        ah, al = halves(state_in[t])
        grad = back[:, at] + in_scale[:, at] * (dot(w_ref[...], ah) + dot(w_ref[...], al))
        back[:, at] = grad
        gh, gl = halves(x_ref[:, at].astype(F32) * grad)
        pick = jnp.where(row16 == 2 * t + lane16 // 64, 1.0, 0.0).astype(BF16)
        gls_ref[...] += dot_nt(pick, gh) + dot_nt(pick, gl)
        return carry

    lax.fori_loop(0, PAIRS, finish, 0)
    collect(1, read_all)
    for i in range(TP):
        gr_ref[i * 32 : (i + 1) * 32] = read_all[i]
    collect(2, late_got)
    acc = late_got[0]
    for i in range(1, TP):
        acc = acc + late_got[i]
    write_part[...] = acc
    gather(3, write_part, write_all)
    for copy in started:
        copy.wait_send()
    for t in range(PAIRS):

        @pl.when(chip != t)
        def _():
            leg(0, t, fwd_chip, fwd_got).wait_send()
            leg(1, t, bwd_chip, bwd_got).wait_send()

    collect(3, write_all)
    for i in range(TP):
        gw_ref[i * 32 : (i + 1) * 32] = write_all[i]


def write_kernel(*refs):
    copies = [
        pltpu.make_async_copy(src, dst, refs[8].at[n])
        for n, (src, dst) in enumerate(zip(refs[0:4], refs[4:8]))
    ]
    for copy in copies:
        copy.start()
    for copy in copies:
        copy.wait()


def on_device(
    query_rows, key_rows, value_rows, mixer_input, write_rows, read_rows, log_step, log_decay
):
    dma = pltpu.SemaphoreType.DMA
    packet = (PAIRS, 2, 72, HD)
    exchange = [
        pltpu.VMEM(packet, F32),
        pltpu.VMEM(packet, F32),
        pltpu.VMEM((PAIRS, 72, HD), F32),
        pltpu.VMEM((CHIPS, 72, HD), F32),
        pltpu.VMEM((CHIPS, 64, HD), F32),
        pltpu.VMEM((2, PAIRS, 64, HD), F32),
    ]
    whole = pl.BlockSpec(memory_space=pl.ANY)
    vmem = pl.BlockSpec(memory_space=pltpu.VMEM)
    wide = (TOK, PAIRS * HD)
    share = (TP, 32, HD)
    held = pl.pallas_call(
        main_kernel,
        out_shape=(
            pltpu.VMEM(wide, F32),
            pltpu.VMEM((TOK, HD), F32),
            pltpu.VMEM((TOK, HD), F32),
            pltpu.VMEM((2 * PAIRS, TOK), F32),
        ),
        in_specs=[whole] * 8,
        out_specs=(vmem,) * 4,
        scratch_shapes=[
            pltpu.VMEM(wide, BF16),
            pltpu.VMEM(wide, BF16),
            pltpu.VMEM((TOK, HD), BF16),
            pltpu.VMEM((TOK, HD), BF16),
            pltpu.VMEM((2 * PAIRS, TOK), F32),
            pltpu.VMEM((2 * PAIRS, TOK), F32),
            pltpu.VMEM((SEQ, TOK, HD), BF16),
            pltpu.VMEM((SEQ, TOK, HD), BF16),
            pltpu.VMEM((SEQ, 8 * TOK, TOK), F32),
            pltpu.VMEM((8 * TOK, HD), F32),
            pltpu.VMEM((2 * TOK, HD), F32),
            pltpu.VMEM((2 * TOK, HD), F32),
            pltpu.VMEM((8 * TOK, HD), BF16),
            pltpu.VMEM((16, TOK, TOK), F32),
            pltpu.VMEM((16, TOK, TOK), BF16),
            pltpu.VMEM((16, TOK, TOK), BF16),
            pltpu.VMEM(wide, F32),
            pltpu.VMEM(wide, F32),
            pltpu.VMEM(wide, F32),
            pltpu.VMEM((HD, TOK), BF16),
            pltpu.VMEM((HD, TOK), BF16),
            pltpu.VMEM((TOK, TOK), F32),
            pltpu.VMEM((TOK, HD), F32),
            *exchange,
            pltpu.VMEM((PAIRS, HD, HD), F32),
            pltpu.VMEM((PAIRS, 2, 64, HD), F32),
            pltpu.VMEM((PAIRS, 2, 64, HD), F32),
            pltpu.VMEM((PAIRS, 64, HD), F32),
            pltpu.VMEM((CHIPS, 64, HD), F32),
            pltpu.VMEM((CHIPS, 64, HD), F32),
            pltpu.VMEM((2, PAIRS, 64, HD), F32),
            pltpu.VMEM(share, F32),
            pltpu.VMEM(share, F32),
            pltpu.VMEM((32, HD), F32),
            pltpu.VMEM(share, F32),
            pltpu.VMEM(share, F32),
            pltpu.VMEM(share, F32),
            pltpu.VMEM((32, HD), F32),
            pltpu.VMEM(share, F32),
            dma((8,)),
            dma((16,)),
            dma((SEQ,)),
            dma((16,)),
            dma((SEQ,)),
            dma((19,)),
            dma((19,)),
            dma((2, CHIPS)),
            dma((2, CHIPS)),
            dma((2, CHIPS)),
            dma((2, CHIPS)),
            dma((4, TP)),
            dma((4, TP)),
        ],
        compiler_params=pltpu.CompilerParams(
            collective_id=0, has_side_effects=True, vmem_limit_bytes=61 * 1024 * 1024
        ),
        name="distill",
    )(query_rows, key_rows, value_rows, mixer_input, write_rows, read_rows, log_step, log_decay)
    return pl.pallas_call(
        write_kernel,
        out_shape=(
            jax.ShapeDtypeStruct(wide, F32),
            jax.ShapeDtypeStruct((TOK, HD), F32),
            jax.ShapeDtypeStruct((TOK, HD), F32),
            jax.ShapeDtypeStruct((2 * PAIRS, TOK), F32),
        ),
        in_specs=[vmem] * 4,
        out_specs=(whole,) * 4,
        scratch_shapes=[dma((4,))],
        compiler_params=pltpu.CompilerParams(vmem_limit_bytes=1024 * 1024),
        name="store",
    )(*held)


def solution(mesh):
    in_specs = (
        P("seq", "tp"),
        P("seq", "tp"),
        P("seq", "tp"),
        P("seq", "tp"),
        P("seq", None),
        P("seq", None),
        P("tp", "seq"),
        P("tp", "seq"),
    )
    out_specs = (P("seq", "tp"), P("seq", None), P("seq", None), P("tp", "seq"))
    return jax.shard_map(
        on_device, mesh=mesh, in_specs=in_specs, out_specs=out_specs, check_vma=False
    )
```
